32 devices in a mesh: gx: 2 (over x), gy: 4 (over z), gz: 4 (over y, core).
Axes of the slice: x: 2, y: 2, z: 4, core: 2. Of those that a mesh axis runs over, the one named last changes fastest.
Arguments:
- fields: float32 [4, 8, 256, 512], P(None, 'gx', 'gy', 'gz'), may hold values from -8 to 8
- volume_code: int32 [8, 256, 512], P('gx', 'gy', 'gz'), may hold values from 65536 to 1048576
- cut_flag: int32 [8, 256, 512], P('gx', 'gy', 'gz'), may hold values 0 or 1
- member_bits: int32 [8, 256, 512], P('gx', 'gy', 'gz'), may hold values from 0 to 134217727
Outputs:
- merged: float32 [4, 8, 256, 512], P(None, 'gx', 'gy', 'gz')
The draws below stay inside these ranges and needn't reach their ends.
All inputs are finite; a program needn't handle non-finite values. No bound on the sum of `cut_flag` on one device may be relied on, other than what follows from the above.
Results may differ from the reference program's by a relative error of at most 0.00015.
Values sent between devices are 32-bit elements; how exact they have to be, the bound alone decides.
A program may use at most 128 MiB of HBM per device.

```python
import jax
import jax.numpy as jnp

FIELDS = 4
PASSES = 2
NX = 8
NY = 256
NZ = 512


def set_ends(result, stream_key, low, largest):
    extent = result.shape
    index_at = [jax.random.randint(jax.random.fold_in(stream_key, axis), (), 0, extent[axis]) for axis in range(len(extent))]
    result = result.at[tuple(index_at)].set(low)
    longest = extent.index(max(extent))
    index_at[longest] = (index_at[longest] + 1) % extent[longest]
    return result.at[tuple(index_at)].set(largest)


def steps_of(stream_key, shape, cuts, low, largest):
    factor_of, own = 1.0, jax.random.fold_in(stream_key, 6)
    for dim, shards_of in cuts:
        draws = jnp.exp(jax.random.uniform(jax.random.fold_in(own, dim), (shards_of,), jnp.float32, low / len(cuts), largest / len(cuts)))
        factor_of = factor_of * jnp.repeat(draws, shape[dim] // shards_of).reshape([-1 if axis == dim else 1 for axis in range(len(shape))])
    return factor_of


def normal_values(key, shape, spread, bound, pieces=(), kind=jnp.bfloat16):
    values = jax.random.normal(key, shape, jnp.float32) * spread
    if len(pieces) > 0:
        values = steps_of(key, shape, pieces, -0.22, 0.18) * values
    return jnp.clip(values, min=-bound, max=bound).astype(kind)


def setup_inputs(seed: int = 0) -> dict:
    streams_of = jax.random.split(jax.random.key(seed), 5)
    return {
        "fields": normal_values(streams_of[0], (FIELDS, NX, NY, NZ), 1.0, 8.0, ((1, 2), (2, 4), (3, 4)), jnp.float32),
        "volume_code": set_ends(jax.random.randint(streams_of[1], (NX, NY, NZ), 65536, 1048577), jax.random.fold_in(streams_of[1], 1), 65536, 1048576).astype(jnp.int32),
        "cut_flag": set_ends((jax.random.randint(streams_of[2], (NX, NY, NZ), 0, 3) < 1).astype(jnp.int32), jax.random.fold_in(streams_of[2], 1), 0, 1),
        "member_bits": set_ends(jax.random.randint(streams_of[3], (NX, NY, NZ), 0, 134217728), jax.random.fold_in(streams_of[3], 1), 0, 134217727).astype(jnp.int32),
    }


def reference(fields, volume_code, cut_flag, member_bits):
    kappa = volume_code.astype(jnp.float32) / 1048576.0
    active = member_bits * cut_flag
    offsets = []
    for dx in (-1, 0, 1):
        for dy in (-1, 0, 1):
            for dz in (-1, 0, 1):
                offsets.append((dx, dy, dz))
    state = fields
    for step in range(PASSES):
        volume = jnp.zeros_like(kappa)
        mass = jnp.zeros_like(fields)
        count = jnp.zeros_like(kappa)
        weighted = kappa[None] * state
        for index, shift in enumerate(offsets):
            if index == 13:
                member = jnp.ones_like(kappa)
            else:
                member = jnp.bitwise_and(jnp.right_shift(active, index), 1).astype(jnp.float32)
            volume = volume + jnp.roll(member * kappa, shift, axis=(0, 1, 2))
            mass = mass + jnp.roll(member[None] * weighted, shift, axis=(1, 2, 3))
        hat = mass / volume[None]
        total = jnp.zeros_like(fields)
        for index, shift in enumerate(offsets):
            if index == 13:
                member = jnp.ones_like(kappa)
            else:
                member = jnp.bitwise_and(jnp.right_shift(active, index), 1).astype(jnp.float32)
            back = (-shift[0], -shift[1], -shift[2])
            total = total + member[None] * jnp.roll(hat, back, axis=(1, 2, 3))
            count = count + member
        state = total / count[None]
    return state
```

```python
import functools

import jax
import jax.numpy as jnp
from jax import lax
from jax.experimental import pallas as pl
from jax.experimental.pallas import tpu as pltpu
from jax.sharding import PartitionSpec as P

PASSES = 2
MESH = pl.DeviceIdType.MESH
AXES = ("gx", "gy", "gz")
SIDES = [(dx, dy) for dx in (-1, 0, 1) for dy in (-1, 0, 1) if (dx, dy) != (0, 0)]
ROWS = 8
SLOT = 8
REACH = 2 * PASSES
GROUP = 4 * REACH


def bit_of(active, dx, dy, dz):
    index = 9 * (dx + 1) + 3 * (dy + 1) + (dz + 1)
    return jnp.bitwise_and(active, 1 << index) != 0


def ones_in(active):
    v = active - jnp.bitwise_and(jnp.right_shift(active, 1), 0x55555555)
    v = jnp.bitwise_and(v, 0x33333333) + jnp.bitwise_and(jnp.right_shift(v, 2), 0x33333333)
    v = jnp.bitwise_and(v + jnp.right_shift(v, 4), 0x0F0F0F0F)
    v = v + jnp.right_shift(v, 8)
    v = v + jnp.right_shift(v, 16)
    return jnp.bitwise_and(v, 63)


def kernel(
    counts, fields, code, flag, bits, out,
    pull0, push0, pull1, push1, act, volume, inverse, acc, total, shifted, packed, landed,
    side_send, side_recv, act_send, act_recv, z_send, z_recv,
):
    nf, nx, ny, nz = fields.shape
    place = [lax.axis_index(name) for name in AXES]

    def device(dx, dy, dz):
        step = (dx, dy, dz)
        return tuple(
            lax.rem(place[d] + step[d] + counts[d], counts[d]) if step[d] else place[d]
            for d in range(3)
        )

    barrier = pltpu.get_barrier_semaphore()
    for dx, dy in SIDES:
        pl.semaphore_signal(barrier, inc=1, device_id=device(dx, dy, 0), device_id_type=MESH)
    for dz in (-1, 1):
        pl.semaphore_signal(barrier, inc=1, device_id=device(0, 0, dz), device_id_type=MESH)

    lane = lax.broadcasted_iota(jnp.int32, (ROWS, nz), 1)
    chunks = ny // ROWS

    def loop_planes(count, work):
        def step(x, carry):
            work(x)
            return carry
        lax.fori_loop(0, count, step, 0)

    def window(side, size, first):
        if side == 0:
            return pl.ds(first, size), pl.ds(first, size)
        if side > 0:
            return pl.ds(first + size - 1, 1), pl.ds(first - 1, 1)
        return pl.ds(first, 1), pl.ds(first + size, 1)

    def side_copies(ref, lead, send, recv):
        copies = []
        for k, (dx, dy) in enumerate(SIDES):
            from_x, to_x = window(dx, nx, 1)
            from_y, to_y = window(dy, ny, ROWS)
            copies.append(
                pltpu.make_async_remote_copy(
                    src_ref=ref.at[lead + (from_x, from_y)],
                    dst_ref=ref.at[lead + (to_x, to_y)],
                    send_sem=send(k),
                    recv_sem=recv(k),
                    device_id=device(dx, dy, 0),
                    device_id_type=MESH,
                )
            )
        return copies

    def z_copies(turn, group, rows):
        copies = []
        for k, dz in enumerate((1, -1)):
            copies.append(
                pltpu.make_async_remote_copy(
                    src_ref=packed.at[turn, group, k, pl.ds(0, rows)],
                    dst_ref=landed.at[turn, group, k, pl.ds(0, rows)],
                    send_sem=z_send.at[turn, group, k],
                    recv_sem=z_recv.at[turn, group, k],
                    device_id=device(0, 0, dz),
                    device_id_type=MESH,
                )
            )
        return copies

    started = []

    def start(copies):
        for copy in copies:
            copy.start()
        started.extend(copies)

    def arrive(copies):
        for copy in copies:
            copy.wait_recv()

    def turn_copies(turn):
        ref = (pull0, push0, pull1, push1)[turn]
        copies = side_copies(
            ref, (slice(None),), lambda k: side_send.at[turn, k], lambda k: side_recv.at[turn, k]
        )
        sides = SIDES
        if turn == 0:
            copies += side_copies(act, (), lambda k: act_send.at[k], lambda k: act_recv.at[k])
            sides = SIDES + SIDES
        across = [copy for copy, side in zip(copies, sides) if side[0] != 0]
        along = [copy for copy, side in zip(copies, sides) if side[0] == 0]
        return across, along

    ends = sorted({0, nx - 1})

    def inner_planes(work):
        if nx > 2:
            def step(x, carry):
                work(x)
                return carry
            lax.fori_loop(1, nx - 1, step, 0)

    def own(x, sign):
        inside = [dx for dx in (-1, 0, 1) if 0 <= x - sign * dx < nx]
        return inside, [dx for dx in (-1, 0, 1) if dx not in inside]

    def rolled(value, amount):
        return pltpu.roll(value, amount % nz, 1)

    def prepare(x):
        for j in range(chunks):
            rows, inner = pl.ds(ROWS * j, ROWS), pl.ds(ROWS * (j + 1), ROWS)
            kappa = code[x, rows].astype(jnp.float32) * (1.0 / 1048576.0)
            active = bits[x, rows] * flag[x, rows]
            act[x + 1, inner] = active
            pull0[0, x + 1, inner] = kappa
            for c in range(nf):
                pull0[c + 1, x + 1, inner] = kappa * fields[c, x, rows]
            others = ones_in(jnp.bitwise_and(active, ((1 << 27) - 1) ^ (1 << 13)))
            inverse[x, rows] = 1.0 / (1 + others).astype(jnp.float32)

    loop_planes(nx, prepare)
    packed[...] = jnp.zeros_like(packed)
    pl.semaphore_wait(barrier, len(SIDES) + 2)
    flights = [turn_copies(turn) for turn in range(2 * PASSES)]
    start(flights[0][1])
    start(flights[0][0])

    def pull(step):
        ref = (pull0, pull1)[step]
        target = (push0, push1)[step]
        arrays = range(nf + 1) if step == 0 else range(1, nf + 1)
        turn = 2 * step
        base = 0 if step == 0 else 1
        across, along = flights[turn]

        def sums(x, j, dxs, dzs, found):
            for dx in dxs:
                for dy in (-1, 0, 1):
                    rows = pl.ds(ROWS * (j + 1) - dy, ROWS)
                    active = act[x + 1 - dx, rows]
                    values = [ref[c - base, x + 1 - dx, rows] for c in arrays]
                    for dz in dzs:
                        if (dx, dy, dz) == (0, 0, 0):
                            terms = values
                        else:
                            member = bit_of(active, dx, dy, dz)
                            terms = [jnp.where(member, v, 0.0) for v in values]
                        if dz in found:
                            found[dz] = [a + b for a, b in zip(found[dz], terms)]
                        else:
                            found[dz] = terms
            return found

        def pack(x, j, found):
            rows = pl.ds(ROWS * j, ROWS)
            for k, dz in enumerate((1, -1)):
                tile = packed[turn, 0, k, rows]
                for c, value in zip(arrays, found[dz]):
                    acc[k, c, x, rows] = value
                    at = x * SLOT + c
                    tile = jnp.where(lane == at, rolled(value, at + (dz == 1)), tile)
                packed[turn, 0, k, rows] = tile

        def early(x, dxs, complete):
            for j in range(chunks):
                rows = pl.ds(ROWS * j, ROWS)
                found = sums(x, j, dxs, (1, 0, -1), {})
                for c, value in zip(arrays, found[0]):
                    total[c, x, rows] = value
                if complete:
                    pack(x, j, found)
                else:
                    for k, dz in enumerate((1, -1)):
                        for c, value in zip(arrays, found[dz]):
                            acc[k, c, x, rows] = value

        arrive(along)
        inner_planes(lambda x: early(x, (-1, 0, 1), True))
        for x in ends:
            early(x, own(x, 1)[0], False)
        arrive(across)
        for x in ends:
            for j in range(chunks):
                rows = pl.ds(ROWS * j, ROWS)
                found = {dz: [acc[k, c, x, rows] for c in arrays] for k, dz in enumerate((1, -1))}
                pack(x, j, sums(x, j, own(x, 1)[1], (1, -1), found))
        copies = z_copies(turn, 0, ny)
        start(copies)
        for x in ends:
            for j in range(chunks):
                rows = pl.ds(ROWS * j, ROWS)
                found = {0: [total[c, x, rows] for c in arrays]}
                for c, value in zip(arrays, sums(x, j, own(x, 1)[1], (0,), found)[0]):
                    total[c, x, rows] = value
        arrive(copies)

        def finish(x):
            for j in range(chunks):
                rows, inner = pl.ds(ROWS * j, ROWS), pl.ds(ROWS * (j + 1), ROWS)
                low, high = landed[turn, 0, 0, rows], landed[turn, 0, 1, rows]
                found = {}
                for c in arrays:
                    at = x * SLOT + c
                    from_low = jnp.where(lane == 0, rolled(low, nz - at), rolled(acc[0, c, x, rows], 1))
                    from_high = jnp.where(
                        lane == nz - 1, rolled(high, nz - 1 - at), rolled(acc[1, c, x, rows], nz - 1)
                    )
                    found[c] = total[c, x, rows] + from_low + from_high
                if step == 0:
                    scale = 1.0 / found[0]
                    volume[x, rows] = scale
                else:
                    scale = volume[x, rows]
                for c in range(nf):
                    target[c, x + 1, inner] = found[c + 1] * scale

        for x in ends:
            finish(x)
        start(flights[turn + 1][0])
        inner_planes(finish)
        start(flights[turn + 1][1])

    def push(step):
        ref = (push0, push1)[step]
        turn = 2 * step + 1
        across, along = flights[turn]

        def columns(group, x):
            for j in range(chunks + 2):
                rows = pl.ds(ROWS * j, ROWS)
                for k, dz in enumerate((1, -1)):
                    tile = packed[turn, group, k, rows]
                    for c in range(nf):
                        at = x * SLOT + c
                        tile = jnp.where(lane == at, rolled(ref[c, x, rows], at + (dz == 1)), tile)
                    packed[turn, group, k, rows] = tile

        def shift(group, x):
            for j in range(chunks + 2):
                rows = pl.ds(ROWS * j, ROWS)
                low, high = landed[turn, group, 0, rows], landed[turn, group, 1, rows]
                for c in range(nf):
                    at = x * SLOT + c
                    value = ref[c, x, rows]
                    shifted[0, c, x, rows] = jnp.where(lane == 0, rolled(low, nz - at), rolled(value, 1))
                    shifted[1, c, x, rows] = jnp.where(
                        lane == nz - 1, rolled(high, nz - 1 - at), rolled(value, nz - 1)
                    )

        def planes(first, count, work):
            def step(x, carry):
                work(x)
                return carry
            lax.fori_loop(first, first + count, step, 0)

        def gathered(x, j, dxs, dzs, values):
            active = act[x + 1, pl.ds(ROWS * (j + 1), ROWS)]
            for dz in dzs:
                for dx in dxs:
                    for dy in (-1, 0, 1):
                        rows = pl.ds(ROWS * (j + 1) + dy, ROWS)
                        if dz == 0:
                            terms = [ref[c, x + 1 + dx, rows] for c in range(nf)]
                        else:
                            terms = [shifted[(dz + 1) // 2, c, x + 1 + dx, rows] for c in range(nf)]
                        if (dx, dy, dz) != (0, 0, 0):
                            member = bit_of(active, dx, dy, dz)
                            terms = [jnp.where(member, v, 0.0) for v in terms]
                        values = terms if values is None else [a + b for a, b in zip(values, terms)]
            return values

        def held(x, j):
            return [total[c, x, pl.ds(ROWS * j, ROWS)] for c in range(nf)]

        def keep(x, j, values):
            for c in range(nf):
                total[c, x, pl.ds(ROWS * j, ROWS)] = values[c]

        def give(x, j, values):
            rows, inner = pl.ds(ROWS * j, ROWS), pl.ds(ROWS * (j + 1), ROWS)
            scale = inverse[x, rows]
            if step == PASSES - 1:
                for c in range(nf):
                    out[c, x, rows] = values[c] * scale
            else:
                scale = scale * pull0[0, x + 1, inner]
                for c in range(nf):
                    pull1[c, x + 1, inner] = values[c] * scale

        def add(x, dxs, dzs, first, last):
            for j in range(chunks):
                values = gathered(x, j, dxs, dzs, None if first else held(x, j))
                (give if last else keep)(x, j, values)

        arrive(along)
        planes(1, nx, lambda x: columns(0, x))
        copies = z_copies(turn, 0, ny + 2 * ROWS)
        start(copies)
        inner_planes(lambda x: add(x, (-1, 0, 1), (0,), True, False))
        for x in ends:
            add(x, own(x, -1)[0], (0,), True, False)
        arrive(copies)
        planes(1, nx, lambda x: shift(0, x))
        for x in ends:
            add(x, own(x, -1)[0], (-1, 1), False, False)
        inner_planes(lambda x: add(x, (-1, 0, 1), (-1, 1), False, True))
        arrive(across)
        for x in (0, nx + 1):
            columns(1, x)
        copies = z_copies(turn, 1, ny + 2 * ROWS)
        start(copies)
        for x in ends:
            add(x, own(x, -1)[1], (0,), False, False)
        arrive(copies)
        for x in (0, nx + 1):
            shift(1, x)
        for x in ends:
            add(x, own(x, -1)[1], (-1, 1), False, True)
        if step < PASSES - 1:
            start(flights[turn + 1][1])
            start(flights[turn + 1][0])

    for step in range(PASSES):
        pull(step)
        push(step)
    for copy in started:
        copy.wait_send()


def body(counts, fields, code, flag, bits):
    nf, nx, ny, nz = fields.shape
    frame = (nx + 2, ny + 2 * ROWS, nz)
    turns = 2 * PASSES
    vmem = pl.BlockSpec(memory_space=pltpu.VMEM)
    f32 = jnp.float32
    return pl.pallas_call(
        functools.partial(kernel, counts),
        out_shape=jax.ShapeDtypeStruct(fields.shape, f32),
        in_specs=[vmem] * 4,
        out_specs=vmem,
        scratch_shapes=[
            pltpu.VMEM((nf + 1,) + frame, f32),
            pltpu.VMEM((nf,) + frame, f32),
            pltpu.VMEM((nf,) + frame, f32),
            pltpu.VMEM((nf,) + frame, f32),
            pltpu.VMEM(frame, jnp.int32),
            pltpu.VMEM((nx, ny, nz), f32),
            pltpu.VMEM((nx, ny, nz), f32),
            pltpu.VMEM((2, nf + 1, nx, ny, nz), f32),
            pltpu.VMEM((nf + 1, nx, ny, nz), f32),
            pltpu.VMEM((2, nf) + frame, f32),
            pltpu.VMEM((turns, 2, 2, ny + 2 * ROWS, nz), f32),
            pltpu.VMEM((turns, 2, 2, ny + 2 * ROWS, nz), f32),
            pltpu.SemaphoreType.DMA((turns, len(SIDES))),
            pltpu.SemaphoreType.DMA((turns, len(SIDES))),
            pltpu.SemaphoreType.DMA((len(SIDES),)),
            pltpu.SemaphoreType.DMA((len(SIDES),)),
            pltpu.SemaphoreType.DMA((turns, 2, 2)),
            pltpu.SemaphoreType.DMA((turns, 2, 2)),
        ],
        compiler_params=pltpu.CompilerParams(collective_id=0, has_side_effects=True),
    )(fields, code, flag, bits)


def folded_kernel(
    counts, fields, code, flag, bits, out,
    raw, rawcode, bit_box, flag_box, act_box, act, pull0, push0, pull1, push1,
    edge_act, edge0, edge1, edge2, edge3, ends, act_ends,
    volume, inverse, weight, edge_volume, edge_weight,
    packed, act_packed, landed, act_landed, done,
    load_sem, x_send, x_recv, y_send, y_recv, z_send, z_recv, back_send, back_recv, own_sem,
):
    nf, nx, ny, nz = fields.shape
    planes = 2 * nx
    half = ny // 2
    tiles = (half + 2 * REACH) // ROWS
    place = [lax.axis_index(name) for name in AXES]
    side = place[0]
    last = ny - REACH
    top, bottom = ROWS, ROWS + REACH + half

    def device(dx, dy, dz):
        step = (dx, dy, dz)
        return tuple(
            lax.rem(place[d] + step[d] + counts[d], counts[d]) if step[d] else place[d]
            for d in range(3)
        )

    def by_side(work):
        for s in (0, 1):
            @pl.when(side == s)
            def _(s=s):
                work(s)

    barrier = pltpu.get_barrier_semaphore()

    def greet(s):
        toward = 1 - 2 * s
        for step in ((1, 0, 0), (0, 1, 0), (0, -1, 0), (1, -toward, 0), (0, 0, 1), (0, 0, -1)):
            pl.semaphore_signal(barrier, inc=1, device_id=device(*step), device_id_type=MESH)

    by_side(greet)

    own_planes, far_planes = pl.ds(0, nx), pl.ds(nx, nx)

    def own_rows(s):
        if s == 0:
            return pl.ds(0, half + REACH), pl.ds(ROWS + REACH, half + REACH)
        return pl.ds(half - REACH, half + REACH), pl.ds(ROWS, half + REACH)

    def loads(s):
        box, place_in = own_rows(s)
        return [
            pltpu.make_async_copy(bits, bit_box, load_sem.at[0]),
            pltpu.make_async_copy(flag, flag_box, load_sem.at[1]),
            pltpu.make_async_copy(fields.at[:, :, box], raw.at[:, own_planes, place_in], load_sem.at[2]),
            pltpu.make_async_copy(code.at[:, box], rawcode.at[own_planes, place_in], load_sem.at[3]),
        ]

    def remote(src, dst, send, recv, step):
        return pltpu.make_async_remote_copy(
            src_ref=src, dst_ref=dst, send_sem=send, recv_sem=recv,
            device_id=device(*step), device_id_type=MESH,
        )

    def triple(from_rows, to_planes, to_rows, send, recv, step):
        return [
            remote(fields.at[:, :, from_rows], raw.at[:, to_planes, to_rows], send.at[0], recv.at[0], step),
            remote(code.at[:, from_rows], rawcode.at[to_planes, to_rows], send.at[1], recv.at[1], step),
            remote(act_box.at[:, from_rows], act.at[0, to_planes, to_rows], send.at[2], recv.at[2], step),
        ]

    def x_rows(s, t):
        if s == 0:
            size = ROWS if t < tiles - 1 else ROWS - REACH
            return pl.ds(half - REACH + ROWS * t, size), pl.ds(ROWS * (t + 1), size)
        if t == 0:
            return pl.ds(0, ROWS - REACH), pl.ds(ROWS + REACH, ROWS - REACH)
        return pl.ds(ROWS * t - REACH, ROWS), pl.ds(ROWS * (t + 1), ROWS)

    def x_copies(s, t):
        from_rows, to_rows = x_rows(s, t)
        return triple(from_rows, far_planes, to_rows, x_send.at[t], x_recv.at[t], (1, 0, 0))

    def y_copies(s, cross):
        low, high = pl.ds(0, REACH), pl.ds(last, REACH)
        up = (s == 0) != cross
        rows, to_rows = (high, pl.ds(top, REACH)) if up else (low, pl.ds(bottom, REACH))
        to_planes = far_planes if cross else own_planes
        step = (1 if cross else 0, 1 if up else -1, 0)
        return triple(rows, to_planes, to_rows, y_send.at[int(cross)], y_recv.at[int(cross)], step)

    def z_copies(t):
        rows = pl.ds(ROWS * t, ROWS)
        copies = []
        for k, dz in enumerate((1, -1)):
            copies.append(remote(
                packed.at[:, rows], landed.at[k, :, rows], z_send.at[t, k, 0], z_recv.at[t, k, 0], (0, 0, dz),
            ))
            copies.append(remote(
                act_packed.at[rows], act_landed.at[k, rows], z_send.at[t, k, 1], z_recv.at[t, k, 1], (0, 0, dz),
            ))
        return copies

    def box_rows(s, k):
        return pl.ds(pl.multiple_of(s * half + ROWS * k, ROWS), ROWS)

    def back_copy(k):
        return remote(
            done.at[k, :, far_planes], out.at[:, :, box_rows(side, k)], back_send.at[k], back_recv.at[k], (1, 0, 0),
        )

    def own_copy(k):
        return pltpu.make_async_copy(done.at[k, :, own_planes], out.at[:, :, box_rows(side, k)], own_sem.at[k])

    lane = lax.broadcasted_iota(jnp.int32, (ROWS, nz), 1)
    within = jnp.bitwise_and(lane, GROUP - 1)
    member_of = jnp.right_shift(lane, GROUP.bit_length() - 1)

    def rolled(value, amount):
        amount %= nz
        return pltpu.roll(value, amount, 1) if amount else value

    def aligned(t):
        return pl.ds(ROWS * (t + 1), ROWS)

    def begin(s):
        copies = loads(s)
        for copy in copies:
            copy.start()
        for copy in copies[:2]:
            copy.wait()
        box, place_in = own_rows(s)

        def plane(x, carry):
            for j in range(ny // ROWS):
                rows = pl.ds(ROWS * j, ROWS)
                act_box[x, rows] = bit_box[x, rows] * flag_box[x, rows]
            return carry

        lax.fori_loop(0, nx, plane, 0)

        pl.semaphore_wait(barrier, 6)
        first, later = y_copies(s, False), y_copies(s, True)
        copies = first + (later if s == 1 else [])
        for t in range(tiles):
            copies += x_copies(s, t)
        for copy in copies + (later if s == 0 else []):
            copy.start()

        def keep(x, carry):
            start, end, size = box.start, place_in.start, box.size
            for j in range(0, size, ROWS):
                n = min(ROWS, size - j)
                act[0, x, pl.ds(end + j, n)] = act_box[x, pl.ds(start + j, n)]
            return carry

        lax.fori_loop(0, nx, keep, 0)
        for copy in loads(s)[2:]:
            copy.wait()

    by_side(begin)

    def arrived(s, t):
        for copy in x_copies(1 - s, t):
            copy.wait_recv()
        if t == (tiles - 1) * s:
            for copy in y_copies(s, False) + y_copies(1 - s, True):
                copy.wait_recv()

    def prepare(t):
        rows = aligned(t)

        def plane(x, carry):
            kappa = rawcode[x, rows].astype(jnp.float32) * (1.0 / 1048576.0)
            pull0[0, 0, x, rows] = kappa
            for c in range(nf):
                pull0[0, c + 1, x, rows] = kappa * raw[c, x, rows]
            others = ones_in(jnp.bitwise_and(act[0, x, rows], ((1 << 27) - 1) ^ (1 << 13)))
            scale = 1.0 / (1 + others).astype(jnp.float32)
            inverse[x, rows] = scale
            weight[x, rows] = scale * kappa
            return carry

        lax.fori_loop(0, planes, plane, 0)
        to = pl.ds(ROWS * t, ROWS)
        for c in range(-1, nf + 1):
            tile = None
            for x in range(planes):
                value = act[0, x, rows] if c < 0 else pull0[0, c, x, rows]
                value = rolled(value, GROUP * x + 2 * REACH)
                tile = value if tile is None else jnp.where(member_of == x, value, tile)
            if c < 0:
                act_packed[to] = tile
            else:
                packed[c, to] = tile
        for copy in z_copies(t):
            copy.start()

    turns = [(sx, sz) for sx in (-1, 0, 1) for sz in (-1, 0, 1)]

    def spread(tile, keep, keep_end):
        for v, (sx, sz) in enumerate(turns):
            keep(v, rolled(tile, -(GROUP * sx + sz)))
        for x in range(planes):
            low = rolled(tile, -(GROUP * x + REACH - 1))
            high = rolled(tile, nz - 1 - (GROUP * x + 3 * REACH))
            keep_end(x, jnp.where(lane == 0, low, high))

    def beside(value, end):
        return (
            jnp.where(lane == 0, end, rolled(value, 1)),
            jnp.where(lane == nz - 1, end, rolled(value, -1)),
        )

    def unpack(t):
        for copy in z_copies(t):
            copy.wait_recv()
        rows, at = aligned(t), pl.ds(ROWS * t, ROWS)

        def joined(own, low, high):
            left = rolled(jnp.where(within < 2 * REACH, low, own), -REACH)
            right = rolled(jnp.where(within < 2 * REACH, own, high), REACH)
            return jnp.where(within < 2 * REACH, left, right)

        tile = joined(act_packed[at], act_landed[0, at], act_landed[1, at])

        def keep(v, value):
            edge_act[v, rows] = value

        def keep_end(x, value):
            act_ends[x] = value

        spread(tile, keep, keep_end)
        others = ones_in(jnp.bitwise_and(tile, ((1 << 27) - 1) ^ (1 << 13)))
        scale = 1.0 / (1 + others).astype(jnp.float32)
        for c in range(nf + 1):
            tile = joined(packed[c, at], landed[0, c, at], landed[1, c, at])
            if c == 0:
                edge_weight[rows] = scale * tile

            def keep(v, value):
                edge0[v, c, rows] = value

            def keep_end(x, value):
                ends[c, x] = value

            spread(tile, keep, keep_end)

        def plane(x, carry):
            low, high = beside(act[0, x, rows], act_ends[x])
            act[1, x, rows], act[2, x, rows] = low, high
            for c in range(nf + 1):
                low, high = beside(pull0[0, c, x, rows], ends[c, x])
                pull0[1, c, x, rows], pull0[2, c, x, rows] = low, high
            return carry

        lax.fori_loop(0, planes, plane, 0, unroll=2)

    def gathered(mask_at, value_at, arrays, pulls):
        values = list(value_at(0, 0, 0))
        center = None if pulls else mask_at(0, 0, 0)
        for sx in (-1, 0, 1):
            for sy in (-1, 0, 1):
                for sz in (-1, 0, 1):
                    if (sx, sy, sz) == (0, 0, 0):
                        continue
                    if pulls:
                        member = bit_of(mask_at(sx, sy, sz), -sx, -sy, -sz)
                    else:
                        member = bit_of(center, sx, sy, sz)
                    terms = value_at(sx, sy, sz)
                    values = [a + jnp.where(member, b, 0.0) for a, b in zip(values, terms)]
        return values

    shifts = {0: 0, -1: 1, 1: 2}

    def edge_values(source, arrays, pulls, first):
        def rows(sy):
            return pl.ds(first + sy, ROWS)

        def mask_at(sx, sy, sz):
            return edge_act[turns.index((sx, sz)), rows(sy)]

        def value_at(sx, sy, sz):
            return [source[turns.index((sx, sz)), c, rows(sy)] for c in range(arrays)]

        return gathered(mask_at, value_at, arrays, pulls)

    def plane_values(source, arrays, pulls, first, x):
        at = {0: x, -1: jnp.where(x == 0, planes - 1, x - 1), 1: jnp.where(x == planes - 1, 0, x + 1)}

        def rows(sy):
            return pl.ds(first + sy, ROWS)

        def mask_at(sx, sy, sz):
            return act[shifts[sz], at[sx], rows(sy)]

        def value_at(sx, sy, sz):
            return [source[shifts[sz], c, at[sx], rows(sy)] for c in range(arrays)]

        return gathered(mask_at, value_at, arrays, pulls)

    def finish(values, stage, read_weight, read_volume, write_volume):
        if stage == 0:
            scale = 1.0 / values[0]
            write_volume(scale)
            values = values[1:]
        elif stage == 1:
            scale = read_weight()
        else:
            scale = read_volume()
        return [value * scale for value in values]

    sources = ((pull0, edge0), (push0, edge1), (pull1, edge2), (push1, edge3))

    def advance(stage, t):
        rows = aligned(t)
        first = ROWS * (t + 1)
        source, edge_source = sources[stage]
        target, edge_target = sources[stage + 1]
        arrays = nf + 1 if stage == 0 else nf
        pulls = stage % 2 == 0

        def write_edge_volume(value):
            edge_volume[rows] = value

        values = edge_values(edge_source, arrays, pulls, first)
        values = finish(
            values, stage, lambda: edge_weight[rows], lambda: edge_volume[rows], write_edge_volume
        )
        for c, value in enumerate(values):
            def keep(v, moved):
                edge_target[v, c, rows] = moved

            def keep_end(x, moved):
                ends[c, x] = moved

            spread(value, keep, keep_end)

        def plane(x, carry):
            def write_volume(value):
                volume[x, rows] = value

            values = plane_values(source, arrays, pulls, first, x)
            values = finish(values, stage, lambda: weight[x, rows], lambda: volume[x, rows], write_volume)
            for c, value in enumerate(values):
                low, high = beside(value, ends[c, x])
                target[0, c, x, rows] = value
                target[1, c, x, rows] = low
                target[2, c, x, rows] = high
            return carry

        lax.fori_loop(0, planes, plane, 0, unroll=2)

    def deliver(k):
        first = ROWS + REACH + ROWS * k

        def plane(x, carry):
            scale = inverse[x, pl.ds(first, ROWS)]
            for c, value in enumerate(plane_values(push1, nf, False, first, x)):
                done[k, c, x] = value * scale
            return carry

        lax.fori_loop(0, planes, plane, 0, unroll=2)
        back_copy(k).start()
        own_copy(k).start()

    for u in range(tiles + 4):
        if u < tiles:
            by_side(functools.partial(lambda t, s: arrived(s, t), u))
            prepare(u)
        if 0 <= u - 1 < tiles:
            unpack(u - 1)
        for stage in range(3):
            if 0 <= u - 2 - stage < tiles:
                advance(stage, u - 2 - stage)
        if 0 <= u - 5:
            deliver(u - 5)

    for t in range(tiles):
        for copy in z_copies(t):
            copy.wait_send()

    def drain(s):
        for copy in y_copies(s, False) + y_copies(s, True):
            copy.wait_send()
        for t in range(tiles):
            for copy in x_copies(s, t):
                copy.wait_send()

    by_side(drain)
    for k in range(tiles - 1):
        own_copy(k).wait()
        back_copy(k).wait()


def folded_body(counts, fields, code, flag, bits):
    nf, nx, ny, nz = fields.shape
    planes = 2 * nx
    depth = ny // 2 + 2 * REACH
    tiles = depth // ROWS
    high = depth + 2 * ROWS
    f32, i32 = jnp.float32, jnp.int32
    whole = pl.BlockSpec(memory_space=pl.ANY)
    dma = pltpu.SemaphoreType.DMA

    def main(n):
        return pltpu.VMEM((3, n, planes, high, nz), f32)

    def edge(n):
        return pltpu.VMEM((9, n, high, nz), f32)

    return pl.pallas_call(
        functools.partial(folded_kernel, counts),
        out_shape=jax.ShapeDtypeStruct(fields.shape, f32),
        in_specs=[whole] * 4,
        out_specs=whole,
        scratch_shapes=[
            pltpu.VMEM((nf, planes, high, nz), f32),
            pltpu.VMEM((planes, high, nz), i32),
            pltpu.VMEM((nx, ny, nz), i32),
            pltpu.VMEM((nx, ny, nz), i32),
            pltpu.VMEM((nx, ny, nz), i32),
            pltpu.VMEM((3, planes, high, nz), i32),
            main(nf + 1), main(nf), main(nf), main(nf),
            pltpu.VMEM((9, high, nz), i32),
            edge(nf + 1), edge(nf), edge(nf), edge(nf),
            pltpu.VMEM((nf + 1, planes, ROWS, nz), f32),
            pltpu.VMEM((planes, ROWS, nz), i32),
            pltpu.VMEM((planes, high, nz), f32),
            pltpu.VMEM((planes, high, nz), f32),
            pltpu.VMEM((planes, high, nz), f32),
            pltpu.VMEM((high, nz), f32),
            pltpu.VMEM((high, nz), f32),
            pltpu.VMEM((nf + 1, depth, nz), f32),
            pltpu.VMEM((depth, nz), i32),
            pltpu.VMEM((2, nf + 1, depth, nz), f32),
            pltpu.VMEM((2, depth, nz), i32),
            pltpu.VMEM((tiles - 1, nf, planes, ROWS, nz), f32),
            dma((4,)),
            dma((tiles, 3)), dma((tiles, 3)),
            dma((2, 3)), dma((2, 3)),
            dma((tiles, 2, 2)), dma((tiles, 2, 2)),
            dma((tiles - 1,)), dma((tiles - 1,)), dma((tiles - 1,)),
        ],
        compiler_params=pltpu.CompilerParams(collective_id=0, has_side_effects=True),
    )(fields, code, flag, bits)


def any_body(counts, fields, code, flag, bits):
    nf, nx, ny, nz = fields.shape
    folds = (
        counts[0] == 2 and min(counts) > 1
        and 2 * nx * GROUP == nz
        and ny % (2 * ROWS) == 0 and ny // 2 >= REACH and 2 * REACH == ROWS
    )
    return (folded_body if folds else body)(counts, fields, code, flag, bits)


def solution(mesh):
    counts = tuple(mesh.shape[name] for name in AXES)
    spec = P("gx", "gy", "gz")
    whole = P(None, "gx", "gy", "gz")
    return jax.shard_map(
        functools.partial(any_body, counts),
        mesh=mesh,
        in_specs=(whole, spec, spec, spec),
        out_specs=whole,
        check_vma=False,
    )
```

```python
import functools

import jax
import jax.numpy as jnp
from jax import lax
from jax.experimental import pallas as pl
from jax.experimental.pallas import tpu as pltpu
from jax.sharding import PartitionSpec as P

PASSES = 2
MESH = pl.DeviceIdType.MESH
AXES = ("gx", "gy", "gz")
SIDES = [(dx, dy) for dx in (-1, 0, 1) for dy in (-1, 0, 1) if (dx, dy) != (0, 0)]
ROWS = 8
SLOT = 8
REACH = 2 * PASSES
GROUP = 4 * REACH


def bit_of(active, dx, dy, dz):
    index = 9 * (dx + 1) + 3 * (dy + 1) + (dz + 1)
    return jnp.bitwise_and(active, 1 << index) != 0


def ones_in(active):
    v = active - jnp.bitwise_and(jnp.right_shift(active, 1), 0x55555555)
    v = jnp.bitwise_and(v, 0x33333333) + jnp.bitwise_and(jnp.right_shift(v, 2), 0x33333333)
    v = jnp.bitwise_and(v + jnp.right_shift(v, 4), 0x0F0F0F0F)
    v = v + jnp.right_shift(v, 8)
    v = v + jnp.right_shift(v, 16)
    return jnp.bitwise_and(v, 63)


def kernel(
    counts, fields, code, flag, bits, out,
    pull0, push0, pull1, push1, act, volume, inverse, acc, total, shifted, packed, landed,
    side_send, side_recv, act_send, act_recv, z_send, z_recv,
):
    nf, nx, ny, nz = fields.shape
    place = [lax.axis_index(name) for name in AXES]

    def device(dx, dy, dz):
        step = (dx, dy, dz)
        return tuple(
            lax.rem(place[d] + step[d] + counts[d], counts[d]) if step[d] else place[d]
            for d in range(3)
        )

    barrier = pltpu.get_barrier_semaphore()
    for dx, dy in SIDES:
        pl.semaphore_signal(barrier, inc=1, device_id=device(dx, dy, 0), device_id_type=MESH)
    for dz in (-1, 1):
        pl.semaphore_signal(barrier, inc=1, device_id=device(0, 0, dz), device_id_type=MESH)

    lane = lax.broadcasted_iota(jnp.int32, (ROWS, nz), 1)
    chunks = ny // ROWS

    def loop_planes(count, work):
        def step(x, carry):
            work(x)
            return carry
        lax.fori_loop(0, count, step, 0)

    def window(side, size, first):
        if side == 0:
            return pl.ds(first, size), pl.ds(first, size)
        if side > 0:
            return pl.ds(first + size - 1, 1), pl.ds(first - 1, 1)
        return pl.ds(first, 1), pl.ds(first + size, 1)

    def side_copies(ref, lead, send, recv):
        copies = []
        for k, (dx, dy) in enumerate(SIDES):
            from_x, to_x = window(dx, nx, 1)
            from_y, to_y = window(dy, ny, ROWS)
            copies.append(
                pltpu.make_async_remote_copy(
                    src_ref=ref.at[lead + (from_x, from_y)],
                    dst_ref=ref.at[lead + (to_x, to_y)],
                    send_sem=send(k),
                    recv_sem=recv(k),
                    device_id=device(dx, dy, 0),
                    device_id_type=MESH,
                )
            )
        return copies

    def z_copies(turn, group, rows):
        copies = []
        for k, dz in enumerate((1, -1)):
            copies.append(
                pltpu.make_async_remote_copy(
                    src_ref=packed.at[turn, group, k, pl.ds(0, rows)],
                    dst_ref=landed.at[turn, group, k, pl.ds(0, rows)],
                    send_sem=z_send.at[turn, group, k],
                    recv_sem=z_recv.at[turn, group, k],
                    device_id=device(0, 0, dz),
                    device_id_type=MESH,
                )
            )
        return copies

    started = []

    def start(copies):
        for copy in copies:
            copy.start()
        started.extend(copies)

    def arrive(copies):
        for copy in copies:
            copy.wait_recv()

    def turn_copies(turn):
        ref = (pull0, push0, pull1, push1)[turn]
        copies = side_copies(
            ref, (slice(None),), lambda k: side_send.at[turn, k], lambda k: side_recv.at[turn, k]
        )
        sides = SIDES
        if turn == 0:
            copies += side_copies(act, (), lambda k: act_send.at[k], lambda k: act_recv.at[k])
            sides = SIDES + SIDES
        across = [copy for copy, side in zip(copies, sides) if side[0] != 0]
        along = [copy for copy, side in zip(copies, sides) if side[0] == 0]
        return across, along

    ends = sorted({0, nx - 1})

    def inner_planes(work):
        if nx > 2:
            def step(x, carry):
                work(x)
                return carry
            lax.fori_loop(1, nx - 1, step, 0)

    def own(x, sign):
        inside = [dx for dx in (-1, 0, 1) if 0 <= x - sign * dx < nx]
        return inside, [dx for dx in (-1, 0, 1) if dx not in inside]

    def rolled(value, amount):
        return pltpu.roll(value, amount % nz, 1)

    def prepare(x):
        for j in range(chunks):
            rows, inner = pl.ds(ROWS * j, ROWS), pl.ds(ROWS * (j + 1), ROWS)
            kappa = code[x, rows].astype(jnp.float32) * (1.0 / 1048576.0)
            active = bits[x, rows] * flag[x, rows]
            act[x + 1, inner] = active
            pull0[0, x + 1, inner] = kappa
            for c in range(nf):
                pull0[c + 1, x + 1, inner] = kappa * fields[c, x, rows]
            others = ones_in(jnp.bitwise_and(active, ((1 << 27) - 1) ^ (1 << 13)))
            inverse[x, rows] = 1.0 / (1 + others).astype(jnp.float32)

    loop_planes(nx, prepare)
    packed[...] = jnp.zeros_like(packed)
    pl.semaphore_wait(barrier, len(SIDES) + 2)
    flights = [turn_copies(turn) for turn in range(2 * PASSES)]
    start(flights[0][1])
    start(flights[0][0])

    def pull(step):
        ref = (pull0, pull1)[step]
        target = (push0, push1)[step]
        arrays = range(nf + 1) if step == 0 else range(1, nf + 1)
        turn = 2 * step
        base = 0 if step == 0 else 1
        across, along = flights[turn]

        def sums(x, j, dxs, dzs, found):
            for dx in dxs:
                for dy in (-1, 0, 1):
                    rows = pl.ds(ROWS * (j + 1) - dy, ROWS)
                    active = act[x + 1 - dx, rows]
                    values = [ref[c - base, x + 1 - dx, rows] for c in arrays]
                    for dz in dzs:
                        if (dx, dy, dz) == (0, 0, 0):
                            terms = values
                        else:
                            member = bit_of(active, dx, dy, dz)
                            terms = [jnp.where(member, v, 0.0) for v in values]
                        if dz in found:
                            found[dz] = [a + b for a, b in zip(found[dz], terms)]
                        else:
                            found[dz] = terms
            return found

        def pack(x, j, found):
            rows = pl.ds(ROWS * j, ROWS)
            for k, dz in enumerate((1, -1)):
                tile = packed[turn, 0, k, rows]
                for c, value in zip(arrays, found[dz]):
                    acc[k, c, x, rows] = value
                    at = x * SLOT + c
                    tile = jnp.where(lane == at, rolled(value, at + (dz == 1)), tile)
                packed[turn, 0, k, rows] = tile

        def early(x, dxs, complete):
            for j in range(chunks):
                rows = pl.ds(ROWS * j, ROWS)
                found = sums(x, j, dxs, (1, 0, -1), {})
                for c, value in zip(arrays, found[0]):
                    total[c, x, rows] = value
                if complete:
                    pack(x, j, found)
                else:
                    for k, dz in enumerate((1, -1)):
                        for c, value in zip(arrays, found[dz]):
                            acc[k, c, x, rows] = value

        arrive(along)
        inner_planes(lambda x: early(x, (-1, 0, 1), True))
        for x in ends:
            early(x, own(x, 1)[0], False)
        arrive(across)
        for x in ends:
            for j in range(chunks):
                rows = pl.ds(ROWS * j, ROWS)
                found = {dz: [acc[k, c, x, rows] for c in arrays] for k, dz in enumerate((1, -1))}
                pack(x, j, sums(x, j, own(x, 1)[1], (1, -1), found))
        copies = z_copies(turn, 0, ny)
        start(copies)
        for x in ends:
            for j in range(chunks):
                rows = pl.ds(ROWS * j, ROWS)
                found = {0: [total[c, x, rows] for c in arrays]}
                for c, value in zip(arrays, sums(x, j, own(x, 1)[1], (0,), found)[0]):
                    total[c, x, rows] = value
        arrive(copies)

        def finish(x):
            for j in range(chunks):
                rows, inner = pl.ds(ROWS * j, ROWS), pl.ds(ROWS * (j + 1), ROWS)
                low, high = landed[turn, 0, 0, rows], landed[turn, 0, 1, rows]
                found = {}
                for c in arrays:
                    at = x * SLOT + c
                    from_low = jnp.where(lane == 0, rolled(low, nz - at), rolled(acc[0, c, x, rows], 1))
                    from_high = jnp.where(
                        lane == nz - 1, rolled(high, nz - 1 - at), rolled(acc[1, c, x, rows], nz - 1)
                    )
                    found[c] = total[c, x, rows] + from_low + from_high
                if step == 0:
                    scale = 1.0 / found[0]
                    volume[x, rows] = scale
                else:
                    scale = volume[x, rows]
                for c in range(nf):
                    target[c, x + 1, inner] = found[c + 1] * scale

        for x in ends:
            finish(x)
        start(flights[turn + 1][0])
        inner_planes(finish)
        start(flights[turn + 1][1])

    def push(step):
        ref = (push0, push1)[step]
        turn = 2 * step + 1
        across, along = flights[turn]

        def columns(group, x):
            for j in range(chunks + 2):
                rows = pl.ds(ROWS * j, ROWS)
                for k, dz in enumerate((1, -1)):
                    tile = packed[turn, group, k, rows]
                    for c in range(nf):
                        at = x * SLOT + c
                        tile = jnp.where(lane == at, rolled(ref[c, x, rows], at + (dz == 1)), tile)
                    packed[turn, group, k, rows] = tile

        def shift(group, x):
            for j in range(chunks + 2):
                rows = pl.ds(ROWS * j, ROWS)
                low, high = landed[turn, group, 0, rows], landed[turn, group, 1, rows]
                for c in range(nf):
                    at = x * SLOT + c
                    value = ref[c, x, rows]
                    shifted[0, c, x, rows] = jnp.where(lane == 0, rolled(low, nz - at), rolled(value, 1))
                    shifted[1, c, x, rows] = jnp.where(
                        lane == nz - 1, rolled(high, nz - 1 - at), rolled(value, nz - 1)
                    )

        def planes(first, count, work):
            def step(x, carry):
                work(x)
                return carry
            lax.fori_loop(first, first + count, step, 0)

        def gathered(x, j, dxs, dzs, values):
            active = act[x + 1, pl.ds(ROWS * (j + 1), ROWS)]
            for dz in dzs:
                for dx in dxs:
                    for dy in (-1, 0, 1):
                        rows = pl.ds(ROWS * (j + 1) + dy, ROWS)
                        if dz == 0:
                            terms = [ref[c, x + 1 + dx, rows] for c in range(nf)]
                        else:
                            terms = [shifted[(dz + 1) // 2, c, x + 1 + dx, rows] for c in range(nf)]
                        if (dx, dy, dz) != (0, 0, 0):
                            member = bit_of(active, dx, dy, dz)
                            terms = [jnp.where(member, v, 0.0) for v in terms]
                        values = terms if values is None else [a + b for a, b in zip(values, terms)]
            return values

        def held(x, j):
            return [total[c, x, pl.ds(ROWS * j, ROWS)] for c in range(nf)]

        def keep(x, j, values):
            for c in range(nf):
                total[c, x, pl.ds(ROWS * j, ROWS)] = values[c]

        def give(x, j, values):
            rows, inner = pl.ds(ROWS * j, ROWS), pl.ds(ROWS * (j + 1), ROWS)
            scale = inverse[x, rows]
            if step == PASSES - 1:
                for c in range(nf):
                    out[c, x, rows] = values[c] * scale
            else:
                scale = scale * pull0[0, x + 1, inner]
                for c in range(nf):
                    pull1[c, x + 1, inner] = values[c] * scale

        def add(x, dxs, dzs, first, last):
            for j in range(chunks):
                values = gathered(x, j, dxs, dzs, None if first else held(x, j))
                (give if last else keep)(x, j, values)

        arrive(along)
        planes(1, nx, lambda x: columns(0, x))
        copies = z_copies(turn, 0, ny + 2 * ROWS)
        start(copies)
        inner_planes(lambda x: add(x, (-1, 0, 1), (0,), True, False))
        for x in ends:
            add(x, own(x, -1)[0], (0,), True, False)
        arrive(copies)
        planes(1, nx, lambda x: shift(0, x))
        for x in ends:
            add(x, own(x, -1)[0], (-1, 1), False, False)
        inner_planes(lambda x: add(x, (-1, 0, 1), (-1, 1), False, True))
        arrive(across)
        for x in (0, nx + 1):
            columns(1, x)
        copies = z_copies(turn, 1, ny + 2 * ROWS)
        start(copies)
        for x in ends:
            add(x, own(x, -1)[1], (0,), False, False)
        arrive(copies)
        for x in (0, nx + 1):
            shift(1, x)
        for x in ends:
            add(x, own(x, -1)[1], (-1, 1), False, True)
        if step < PASSES - 1:
            start(flights[turn + 1][1])
            start(flights[turn + 1][0])

    for step in range(PASSES):
        pull(step)
        push(step)
    for copy in started:
        copy.wait_send()


def body(counts, fields, code, flag, bits):
    nf, nx, ny, nz = fields.shape
    frame = (nx + 2, ny + 2 * ROWS, nz)
    turns = 2 * PASSES
    vmem = pl.BlockSpec(memory_space=pltpu.VMEM)
    f32 = jnp.float32
    return pl.pallas_call(
        functools.partial(kernel, counts),
        out_shape=jax.ShapeDtypeStruct(fields.shape, f32),
        in_specs=[vmem] * 4,
        out_specs=vmem,
        scratch_shapes=[
            pltpu.VMEM((nf + 1,) + frame, f32),
            pltpu.VMEM((nf,) + frame, f32),
            pltpu.VMEM((nf,) + frame, f32),
            pltpu.VMEM((nf,) + frame, f32),
            pltpu.VMEM(frame, jnp.int32),
            pltpu.VMEM((nx, ny, nz), f32),
            pltpu.VMEM((nx, ny, nz), f32),
            pltpu.VMEM((2, nf + 1, nx, ny, nz), f32),
            pltpu.VMEM((nf + 1, nx, ny, nz), f32),
            pltpu.VMEM((2, nf) + frame, f32),
            pltpu.VMEM((turns, 2, 2, ny + 2 * ROWS, nz), f32),
            pltpu.VMEM((turns, 2, 2, ny + 2 * ROWS, nz), f32),
            pltpu.SemaphoreType.DMA((turns, len(SIDES))),
            pltpu.SemaphoreType.DMA((turns, len(SIDES))),
            pltpu.SemaphoreType.DMA((len(SIDES),)),
            pltpu.SemaphoreType.DMA((len(SIDES),)),
            pltpu.SemaphoreType.DMA((turns, 2, 2)),
            pltpu.SemaphoreType.DMA((turns, 2, 2)),
        ],
        compiler_params=pltpu.CompilerParams(collective_id=0, has_side_effects=True),
    )(fields, code, flag, bits)


def folded_kernel(
    counts, fields, code, flag, bits, out,
    raw, rawcode, bit_box, flag_box, act_box, act, pull0, push0, pull1, push1,
    edge_act, edge0, edge1, edge2, edge3, ends, act_ends,
    volume, inverse, weight, edge_volume, edge_weight,
    packed, act_packed, landed, act_landed, done,
    load_sem, x_send, x_recv, y_send, y_recv, z_send, z_recv, back_send, back_recv, own_sem,
):
    nf, nx, ny, nz = fields.shape
    planes = 2 * nx
    half = ny // 2
    tiles = (half + 2 * REACH) // ROWS
    place = [lax.axis_index(name) for name in AXES]
    side = place[0]
    last = ny - REACH
    top, bottom = ROWS, ROWS + REACH + half

    def device(dx, dy, dz):
        step = (dx, dy, dz)
        return tuple(
            lax.rem(place[d] + step[d] + counts[d], counts[d]) if step[d] else place[d]
            for d in range(3)
        )

    def by_side(work):
        for s in (0, 1):
            @pl.when(side == s)
            def _(s=s):
                work(s)

    barrier = pltpu.get_barrier_semaphore()

    def greet(s):
        toward = 1 - 2 * s
        for step in ((1, 0, 0), (0, 1, 0), (0, -1, 0), (1, -toward, 0), (0, 0, 1), (0, 0, -1)):
            pl.semaphore_signal(barrier, inc=1, device_id=device(*step), device_id_type=MESH)

    by_side(greet)

    own_planes, far_planes = pl.ds(0, nx), pl.ds(nx, nx)

    def own_rows(s):
        if s == 0:
            return pl.ds(0, half + REACH), pl.ds(ROWS + REACH, half + REACH)
        return pl.ds(half - REACH, half + REACH), pl.ds(ROWS, half + REACH)

    def loads(s):
        box, place_in = own_rows(s)
        return [
            pltpu.make_async_copy(bits, bit_box, load_sem.at[0]),
            pltpu.make_async_copy(flag, flag_box, load_sem.at[1]),
            pltpu.make_async_copy(fields.at[:, :, box], raw.at[:, own_planes, place_in], load_sem.at[2]),
            pltpu.make_async_copy(code.at[:, box], rawcode.at[own_planes, place_in], load_sem.at[3]),
        ]

    def remote(src, dst, send, recv, step):
        return pltpu.make_async_remote_copy(
            src_ref=src, dst_ref=dst, send_sem=send, recv_sem=recv,
            device_id=device(*step), device_id_type=MESH,
        )

    def triple(from_rows, to_planes, to_rows, send, recv, step):
        return [
            remote(fields.at[:, :, from_rows], raw.at[:, to_planes, to_rows], send.at[0], recv.at[0], step),
            remote(code.at[:, from_rows], rawcode.at[to_planes, to_rows], send.at[1], recv.at[1], step),
            remote(act_box.at[:, from_rows], act.at[0, to_planes, to_rows], send.at[2], recv.at[2], step),
        ]

    def x_rows(s, t):
        if s == 0:
            size = ROWS if t < tiles - 1 else ROWS - REACH
            return pl.ds(half - REACH + ROWS * t, size), pl.ds(ROWS * (t + 1), size)
        if t == 0:
            return pl.ds(0, ROWS - REACH), pl.ds(ROWS + REACH, ROWS - REACH)
        return pl.ds(ROWS * t - REACH, ROWS), pl.ds(ROWS * (t + 1), ROWS)

    def x_copies(s, t):
        from_rows, to_rows = x_rows(s, t)
        return triple(from_rows, far_planes, to_rows, x_send.at[t], x_recv.at[t], (1, 0, 0))

    def y_copies(s, cross):
        low, high = pl.ds(0, REACH), pl.ds(last, REACH)
        up = (s == 0) != cross
        rows, to_rows = (high, pl.ds(top, REACH)) if up else (low, pl.ds(bottom, REACH))
        to_planes = far_planes if cross else own_planes
        step = (1 if cross else 0, 1 if up else -1, 0)
        return triple(rows, to_planes, to_rows, y_send.at[int(cross)], y_recv.at[int(cross)], step)

    def z_copies(t):
        rows = pl.ds(pl.multiple_of(ROWS * t, ROWS), ROWS)
        copies = []
        for k, dz in enumerate((1, -1)):
            copies.append(remote(
                packed.at[:, rows], landed.at[k, :, rows], z_send.at[t, k, 0], z_recv.at[t, k, 0], (0, 0, dz),
            ))
            copies.append(remote(
                act_packed.at[rows], act_landed.at[k, rows], z_send.at[t, k, 1], z_recv.at[t, k, 1], (0, 0, dz),
            ))
        return copies

    def box_rows(s, k):
        return pl.ds(pl.multiple_of(s * half + ROWS * k, ROWS), ROWS)

    def back_copy(k):
        return remote(
            done.at[k, :, far_planes], out.at[:, :, box_rows(side, k)], back_send.at[k], back_recv.at[k], (1, 0, 0),
        )

    def own_copy(k):
        return pltpu.make_async_copy(done.at[k, :, own_planes], out.at[:, :, box_rows(side, k)], own_sem.at[k])

    lane = lax.broadcasted_iota(jnp.int32, (ROWS, nz), 1)
    within = jnp.bitwise_and(lane, GROUP - 1)
    member_of = jnp.right_shift(lane, GROUP.bit_length() - 1)

    def rolled(value, amount):
        amount %= nz
        return pltpu.roll(value, amount, 1) if amount else value

    def begin(s):
        copies = loads(s)
        for copy in copies:
            copy.start()
        for copy in copies[:2]:
            copy.wait()
        box, place_in = own_rows(s)

        def plane(x, carry):
            for j in range(ny // ROWS):
                rows = pl.ds(ROWS * j, ROWS)
                act_box[x, rows] = bit_box[x, rows] * flag_box[x, rows]
            return carry

        lax.fori_loop(0, nx, plane, 0)

        pl.semaphore_wait(barrier, 6)
        first, later = y_copies(s, False), y_copies(s, True)
        copies = first + (later if s == 1 else [])
        for t in range(tiles):
            copies += x_copies(s, t)
        for copy in copies + (later if s == 0 else []):
            copy.start()

        def keep(x, carry):
            start, end, size = box.start, place_in.start, box.size
            for j in range(0, size, ROWS):
                n = min(ROWS, size - j)
                act[0, x, pl.ds(end + j, n)] = act_box[x, pl.ds(start + j, n)]
            return carry

        lax.fori_loop(0, nx, keep, 0)
        for copy in loads(s)[2:]:
            copy.wait()

    by_side(begin)

    def arrived(t):
        short = t == (tiles - 1) * side

        def wait_rows(size):
            rows = pl.ds(0, size)
            for copy in triple(rows, far_planes, rows, x_send.at[t], x_recv.at[t], (1, 0, 0)):
                copy.wait_recv()

        @pl.when(short)
        def _():
            wait_rows(ROWS - REACH)
            for cross in (False, True):
                for copy in y_copies(0, cross):
                    copy.wait_recv()

        @pl.when(jnp.logical_not(short))
        def _():
            wait_rows(ROWS)

    def view(ref, t, *lead):
        return ref.at[(*lead, pl.ds(pl.multiple_of(ROWS * t, ROWS), 3 * ROWS))]

    def get(ref, t, offset, *lead):
        return view(ref, t, *lead)[pl.ds(offset, ROWS)]

    def put(ref, t, offset, *lead):
        def write(value):
            view(ref, t, *lead)[pl.ds(offset, ROWS)] = value
        return write

    def strip(t):
        return pl.ds(pl.multiple_of(ROWS * t, ROWS), ROWS)

    def prepare(t):
        def plane(x, carry):
            kappa = get(rawcode, t, ROWS, x).astype(jnp.float32) * (1.0 / 1048576.0)
            put(pull0, t, ROWS, 0, x, 0)(kappa)
            for c in range(nf):
                put(pull0, t, ROWS, 0, x, c + 1)(kappa * get(raw, t, ROWS, c, x))
            others = ones_in(jnp.bitwise_and(get(act, t, ROWS, 0, x), ((1 << 27) - 1) ^ (1 << 13)))
            scale = 1.0 / (1 + others).astype(jnp.float32)
            put(inverse, t, ROWS, x)(scale)
            put(weight, t, ROWS, x)(scale * kappa)
            return carry

        lax.fori_loop(0, planes, plane, 0, unroll=8)
        for c in range(-1, nf + 1):
            tile = None
            for x in range(planes):
                value = get(act, t, ROWS, 0, x) if c < 0 else get(pull0, t, ROWS, 0, x, c)
                value = rolled(value, GROUP * x + 2 * REACH)
                tile = value if tile is None else jnp.where(member_of == x, value, tile)
            if c < 0:
                act_packed[strip(t)] = tile
            else:
                packed[c, strip(t)] = tile
        for copy in z_copies(t):
            copy.start()

    turns = [(sx, sz) for sx in (-1, 0, 1) for sz in (-1, 0, 1)]

    def spread(tile, keep, keep_end):
        for v, (sx, sz) in enumerate(turns):
            keep(v)(rolled(tile, -(GROUP * sx + sz)))
        meet = 3 * REACH + 1
        pair = jnp.where(within == meet, rolled(tile, meet - (REACH - 1)), tile)
        for x in range(planes):
            keep_end(x, rolled(pair, -(GROUP * x + meet)))

    def beside(value, end):
        return (
            jnp.where(lane == 0, end, rolled(value, 1)),
            jnp.where(lane == nz - 1, end, rolled(value, -1)),
        )

    def unpack(t):
        for copy in z_copies(t):
            copy.wait_recv()
        at = strip(t)

        def joined(own, low, high):
            left = rolled(jnp.where(within < 2 * REACH, low, own), -REACH)
            right = rolled(jnp.where(within < 2 * REACH, own, high), REACH)
            return jnp.where(within < 2 * REACH, left, right)

        tile = joined(act_packed[at], act_landed[0, at], act_landed[1, at])

        def keep_end(x, value):
            act_ends[x] = value

        spread(tile, lambda v: put(edge_act, t, ROWS, v), keep_end)
        others = ones_in(jnp.bitwise_and(tile, ((1 << 27) - 1) ^ (1 << 13)))
        scale = 1.0 / (1 + others).astype(jnp.float32)
        for c in range(nf + 1):
            tile = joined(packed[c, at], landed[0, c, at], landed[1, c, at])
            if c == 0:
                put(edge_weight, t, ROWS)(scale * tile)

            def keep_end(x, value):
                ends[x, c] = value

            spread(tile, lambda v: put(edge0, t, ROWS, v, c), keep_end)

        def plane(x, carry):
            low, high = beside(get(act, t, ROWS, 0, x), act_ends[x])
            put(act, t, ROWS, 1, x)(low)
            put(act, t, ROWS, 2, x)(high)
            for c in range(nf + 1):
                low, high = beside(get(pull0, t, ROWS, 0, x, c), ends[x, c])
                put(pull0, t, ROWS, 1, x, c)(low)
                put(pull0, t, ROWS, 2, x, c)(high)
            return carry

        lax.fori_loop(0, planes, plane, 0, unroll=8)

    def gathered(mask_at, value_at, arrays, pulls):
        values = list(value_at(0, 0, 0))
        center = None if pulls else mask_at(0, 0, 0)
        for sx in (-1, 0, 1):
            for sy in (-1, 0, 1):
                for sz in (-1, 0, 1):
                    if (sx, sy, sz) == (0, 0, 0):
                        continue
                    if pulls:
                        member = bit_of(mask_at(sx, sy, sz), -sx, -sy, -sz)
                    else:
                        member = bit_of(center, sx, sy, sz)
                    terms = value_at(sx, sy, sz)
                    values = [a + jnp.where(member, b, 0.0) for a, b in zip(values, terms)]
        return values

    shifts = {0: 0, -1: 1, 1: 2}

    def edge_values(source, arrays, pulls, t, first):
        def mask_at(sx, sy, sz):
            return get(edge_act, t, first + sy, turns.index((sx, sz)))

        def value_at(sx, sy, sz):
            return [get(source, t, first + sy, turns.index((sx, sz)), c) for c in range(arrays)]

        return gathered(mask_at, value_at, arrays, pulls)

    def plane_values(source, arrays, pulls, t, first, x):
        at = {0: x, -1: jnp.where(x == 0, planes - 1, x - 1), 1: jnp.where(x == planes - 1, 0, x + 1)}

        def mask_at(sx, sy, sz):
            return get(act, t, first + sy, shifts[sz], at[sx])

        def value_at(sx, sy, sz):
            return [get(source, t, first + sy, shifts[sz], at[sx], c) for c in range(arrays)]

        return gathered(mask_at, value_at, arrays, pulls)

    def finish(values, stage, read_weight, read_volume, write_volume):
        if stage == 0:
            scale = 1.0 / values[0]
            write_volume(scale)
            values = values[1:]
        elif stage == 1:
            scale = read_weight()
        else:
            scale = read_volume()
        return [value * scale for value in values]

    sources = ((pull0, edge0), (push0, edge1), (pull1, edge2), (push1, edge3))

    def advance(stage, t):
        first = ROWS - 1 - stage
        source, edge_source = sources[stage]
        target, edge_target = sources[stage + 1]
        arrays = nf + 1 if stage == 0 else nf
        pulls = stage % 2 == 0
        values = edge_values(edge_source, arrays, pulls, t, first)
        values = finish(
            values, stage, lambda: get(edge_weight, t, first),
            lambda: get(edge_volume, t, first), put(edge_volume, t, first),
        )
        for c, value in enumerate(values):
            def keep_end(x, moved):
                ends[x, c] = moved

            spread(value, lambda v: put(edge_target, t, first, v, c), keep_end)

        def plane(x, carry):
            values = plane_values(source, arrays, pulls, t, first, x)
            values = finish(
                values, stage, lambda: get(weight, t, first, x),
                lambda: get(volume, t, first, x), put(volume, t, first, x),
            )
            for c, value in enumerate(values):
                low, high = beside(value, ends[x, c])
                put(target, t, first, 0, x, c)(value)
                put(target, t, first, 1, x, c)(low)
                put(target, t, first, 2, x, c)(high)
            return carry

        lax.fori_loop(0, planes, plane, 0, unroll=8)

    def deliver(t):
        k = t - 1
        first = REACH

        def plane(x, carry):
            scale = get(inverse, t, first, x)
            for c, value in enumerate(plane_values(push1, nf, False, t, first, x)):
                done[k, c, x] = value * scale
            return carry

        lax.fori_loop(0, planes, plane, 0, unroll=8)
        back_copy(k).start()
        own_copy(k).start()

    def step(u, carry):
        @pl.when(u < tiles)
        def _():
            arrived(u)
            prepare(u)

        @pl.when(u > 0)
        def _():
            unpack(u - 1)
            for stage in range(3):
                advance(stage, u - 1)

        @pl.when(u > 1)
        def _():
            deliver(u - 1)

        return carry

    lax.fori_loop(0, tiles + 1, step, 0)

    for t in range(tiles):
        for copy in z_copies(t):
            copy.wait_send()

    def drain(s):
        for copy in y_copies(s, False) + y_copies(s, True):
            copy.wait_send()
        for t in range(tiles):
            for copy in x_copies(s, t):
                copy.wait_send()

    by_side(drain)
    for k in range(tiles - 1):
        own_copy(k).wait()
        back_copy(k).wait()


def folded_body(counts, fields, code, flag, bits):
    nf, nx, ny, nz = fields.shape
    planes = 2 * nx
    depth = ny // 2 + 2 * REACH
    tiles = depth // ROWS
    high = depth + 2 * ROWS
    f32, i32 = jnp.float32, jnp.int32
    whole = pl.BlockSpec(memory_space=pl.ANY)
    dma = pltpu.SemaphoreType.DMA

    def main(n):
        return pltpu.VMEM((3, planes, n, high, nz), f32)

    def edge(n):
        return pltpu.VMEM((9, n, high, nz), f32)

    return pl.pallas_call(
        functools.partial(folded_kernel, counts),
        out_shape=jax.ShapeDtypeStruct(fields.shape, f32),
        in_specs=[whole] * 4,
        out_specs=whole,
        scratch_shapes=[
            pltpu.VMEM((nf, planes, high, nz), f32),
            pltpu.VMEM((planes, high, nz), i32),
            pltpu.VMEM((nx, ny, nz), i32),
            pltpu.VMEM((nx, ny, nz), i32),
            pltpu.VMEM((nx, ny, nz), i32),
            pltpu.VMEM((3, planes, high, nz), i32),
            main(nf + 1), main(nf), main(nf), main(nf),
            pltpu.VMEM((9, high, nz), i32),
            edge(nf + 1), edge(nf), edge(nf), edge(nf),
            pltpu.VMEM((planes, nf + 1, ROWS, nz), f32),
            pltpu.VMEM((planes, ROWS, nz), i32),
            pltpu.VMEM((planes, high, nz), f32),
            pltpu.VMEM((planes, high, nz), f32),
            pltpu.VMEM((planes, high, nz), f32),
            pltpu.VMEM((high, nz), f32),
            pltpu.VMEM((high, nz), f32),
            pltpu.VMEM((nf + 1, depth, nz), f32),
            pltpu.VMEM((depth, nz), i32),
            pltpu.VMEM((2, nf + 1, depth, nz), f32),
            pltpu.VMEM((2, depth, nz), i32),
            pltpu.VMEM((tiles - 1, nf, planes, ROWS, nz), f32),
            dma((4,)),
            dma((tiles, 3)), dma((tiles, 3)),
            dma((2, 3)), dma((2, 3)),
            dma((tiles, 2, 2)), dma((tiles, 2, 2)),
            dma((tiles - 1,)), dma((tiles - 1,)), dma((tiles - 1,)),
        ],
        compiler_params=pltpu.CompilerParams(collective_id=0, has_side_effects=True),
    )(fields, code, flag, bits)


def any_body(counts, fields, code, flag, bits):
    nf, nx, ny, nz = fields.shape
    folds = (
        counts[0] == 2 and min(counts) > 1
        and 2 * nx * GROUP == nz
        and ny % (2 * ROWS) == 0 and ny // 2 >= REACH and 2 * REACH == ROWS
    )
    return (folded_body if folds else body)(counts, fields, code, flag, bits)


def solution(mesh):
    counts = tuple(mesh.shape[name] for name in AXES)
    spec = P("gx", "gy", "gz")
    whole = P(None, "gx", "gy", "gz")
    return jax.shard_map(
        functools.partial(any_body, counts),
        mesh=mesh,
        in_specs=(whole, spec, spec, spec),
        out_specs=whole,
        check_vma=False,
    )
```

```python
import functools

import jax
import jax.numpy as jnp
from jax import lax
from jax.experimental import pallas as pl
from jax.experimental.pallas import tpu as pltpu
from jax.sharding import PartitionSpec as P

PASSES = 2
MESH = pl.DeviceIdType.MESH
AXES = ("gx", "gy", "gz")
SIDES = [(dx, dy) for dx in (-1, 0, 1) for dy in (-1, 0, 1) if (dx, dy) != (0, 0)]
ROWS = 8
SLOT = 8
REACH = 2 * PASSES
GROUP = 4 * REACH


def bit_of(active, dx, dy, dz):
    index = 9 * (dx + 1) + 3 * (dy + 1) + (dz + 1)
    return jnp.bitwise_and(active, 1 << index) != 0


def ones_in(active):
    v = active - jnp.bitwise_and(jnp.right_shift(active, 1), 0x55555555)
    v = jnp.bitwise_and(v, 0x33333333) + jnp.bitwise_and(jnp.right_shift(v, 2), 0x33333333)
    v = jnp.bitwise_and(v + jnp.right_shift(v, 4), 0x0F0F0F0F)
    v = v + jnp.right_shift(v, 8)
    v = v + jnp.right_shift(v, 16)
    return jnp.bitwise_and(v, 63)


def kernel(
    counts, fields, code, flag, bits, out,
    pull0, push0, pull1, push1, act, volume, inverse, acc, total, shifted, packed, landed,
    side_send, side_recv, act_send, act_recv, z_send, z_recv,
):
    nf, nx, ny, nz = fields.shape
    place = [lax.axis_index(name) for name in AXES]

    def device(dx, dy, dz):
        step = (dx, dy, dz)
        return tuple(
            lax.rem(place[d] + step[d] + counts[d], counts[d]) if step[d] else place[d]
            for d in range(3)
        )

    barrier = pltpu.get_barrier_semaphore()
    for dx, dy in SIDES:
        pl.semaphore_signal(barrier, inc=1, device_id=device(dx, dy, 0), device_id_type=MESH)
    for dz in (-1, 1):
        pl.semaphore_signal(barrier, inc=1, device_id=device(0, 0, dz), device_id_type=MESH)

    lane = lax.broadcasted_iota(jnp.int32, (ROWS, nz), 1)
    chunks = ny // ROWS

    def loop_planes(count, work):
        def step(x, carry):
            work(x)
            return carry
        lax.fori_loop(0, count, step, 0)

    def window(side, size, first):
        if side == 0:
            return pl.ds(first, size), pl.ds(first, size)
        if side > 0:
            return pl.ds(first + size - 1, 1), pl.ds(first - 1, 1)
        return pl.ds(first, 1), pl.ds(first + size, 1)

    def side_copies(ref, lead, send, recv):
        copies = []
        for k, (dx, dy) in enumerate(SIDES):
            from_x, to_x = window(dx, nx, 1)
            from_y, to_y = window(dy, ny, ROWS)
            copies.append(
                pltpu.make_async_remote_copy(
                    src_ref=ref.at[lead + (from_x, from_y)],
                    dst_ref=ref.at[lead + (to_x, to_y)],
                    send_sem=send(k),
                    recv_sem=recv(k),
                    device_id=device(dx, dy, 0),
                    device_id_type=MESH,
                )
            )
        return copies

    def z_copies(turn, group, rows):
        copies = []
        for k, dz in enumerate((1, -1)):
            copies.append(
                pltpu.make_async_remote_copy(
                    src_ref=packed.at[turn, group, k, pl.ds(0, rows)],
                    dst_ref=landed.at[turn, group, k, pl.ds(0, rows)],
                    send_sem=z_send.at[turn, group, k],
                    recv_sem=z_recv.at[turn, group, k],
                    device_id=device(0, 0, dz),
                    device_id_type=MESH,
                )
            )
        return copies

    started = []

    def start(copies):
        for copy in copies:
            copy.start()
        started.extend(copies)

    def arrive(copies):
        for copy in copies:
            copy.wait_recv()

    def turn_copies(turn):
        ref = (pull0, push0, pull1, push1)[turn]
        copies = side_copies(
            ref, (slice(None),), lambda k: side_send.at[turn, k], lambda k: side_recv.at[turn, k]
        )
        sides = SIDES
        if turn == 0:
            copies += side_copies(act, (), lambda k: act_send.at[k], lambda k: act_recv.at[k])
            sides = SIDES + SIDES
        across = [copy for copy, side in zip(copies, sides) if side[0] != 0]
        along = [copy for copy, side in zip(copies, sides) if side[0] == 0]
        return across, along

    ends = sorted({0, nx - 1})

    def inner_planes(work):
        if nx > 2:
            def step(x, carry):
                work(x)
                return carry
            lax.fori_loop(1, nx - 1, step, 0)

    def own(x, sign):
        inside = [dx for dx in (-1, 0, 1) if 0 <= x - sign * dx < nx]
        return inside, [dx for dx in (-1, 0, 1) if dx not in inside]

    def rolled(value, amount):
        return pltpu.roll(value, amount % nz, 1)

    def prepare(x):
        for j in range(chunks):
            rows, inner = pl.ds(ROWS * j, ROWS), pl.ds(ROWS * (j + 1), ROWS)
            kappa = code[x, rows].astype(jnp.float32) * (1.0 / 1048576.0)
            active = bits[x, rows] * flag[x, rows]
            act[x + 1, inner] = active
            pull0[0, x + 1, inner] = kappa
            for c in range(nf):
                pull0[c + 1, x + 1, inner] = kappa * fields[c, x, rows]
            others = ones_in(jnp.bitwise_and(active, ((1 << 27) - 1) ^ (1 << 13)))
            inverse[x, rows] = 1.0 / (1 + others).astype(jnp.float32)

    loop_planes(nx, prepare)
    packed[...] = jnp.zeros_like(packed)
    pl.semaphore_wait(barrier, len(SIDES) + 2)
    flights = [turn_copies(turn) for turn in range(2 * PASSES)]
    start(flights[0][1])
    start(flights[0][0])

    def pull(step):
        ref = (pull0, pull1)[step]
        target = (push0, push1)[step]
        arrays = range(nf + 1) if step == 0 else range(1, nf + 1)
        turn = 2 * step
        base = 0 if step == 0 else 1
        across, along = flights[turn]

        def sums(x, j, dxs, dzs, found):
            for dx in dxs:
                for dy in (-1, 0, 1):
                    rows = pl.ds(ROWS * (j + 1) - dy, ROWS)
                    active = act[x + 1 - dx, rows]
                    values = [ref[c - base, x + 1 - dx, rows] for c in arrays]
                    for dz in dzs:
                        if (dx, dy, dz) == (0, 0, 0):
                            terms = values
                        else:
                            member = bit_of(active, dx, dy, dz)
                            terms = [jnp.where(member, v, 0.0) for v in values]
                        if dz in found:
                            found[dz] = [a + b for a, b in zip(found[dz], terms)]
                        else:
                            found[dz] = terms
            return found

        def pack(x, j, found):
            rows = pl.ds(ROWS * j, ROWS)
            for k, dz in enumerate((1, -1)):
                tile = packed[turn, 0, k, rows]
                for c, value in zip(arrays, found[dz]):
                    acc[k, c, x, rows] = value
                    at = x * SLOT + c
                    tile = jnp.where(lane == at, rolled(value, at + (dz == 1)), tile)
                packed[turn, 0, k, rows] = tile

        def early(x, dxs, complete):
            for j in range(chunks):
                rows = pl.ds(ROWS * j, ROWS)
                found = sums(x, j, dxs, (1, 0, -1), {})
                for c, value in zip(arrays, found[0]):
                    total[c, x, rows] = value
                if complete:
                    pack(x, j, found)
                else:
                    for k, dz in enumerate((1, -1)):
                        for c, value in zip(arrays, found[dz]):
                            acc[k, c, x, rows] = value

        arrive(along)
        inner_planes(lambda x: early(x, (-1, 0, 1), True))
        for x in ends:
            early(x, own(x, 1)[0], False)
        arrive(across)
        for x in ends:
            for j in range(chunks):
                rows = pl.ds(ROWS * j, ROWS)
                found = {dz: [acc[k, c, x, rows] for c in arrays] for k, dz in enumerate((1, -1))}
                pack(x, j, sums(x, j, own(x, 1)[1], (1, -1), found))
        copies = z_copies(turn, 0, ny)
        start(copies)
        for x in ends:
            for j in range(chunks):
                rows = pl.ds(ROWS * j, ROWS)
                found = {0: [total[c, x, rows] for c in arrays]}
                for c, value in zip(arrays, sums(x, j, own(x, 1)[1], (0,), found)[0]):
                    total[c, x, rows] = value
        arrive(copies)

        def finish(x):
            for j in range(chunks):
                rows, inner = pl.ds(ROWS * j, ROWS), pl.ds(ROWS * (j + 1), ROWS)
                low, high = landed[turn, 0, 0, rows], landed[turn, 0, 1, rows]
                found = {}
                for c in arrays:
                    at = x * SLOT + c
                    from_low = jnp.where(lane == 0, rolled(low, nz - at), rolled(acc[0, c, x, rows], 1))
                    from_high = jnp.where(
                        lane == nz - 1, rolled(high, nz - 1 - at), rolled(acc[1, c, x, rows], nz - 1)
                    )
                    found[c] = total[c, x, rows] + from_low + from_high
                if step == 0:
                    scale = 1.0 / found[0]
                    volume[x, rows] = scale
                else:
                    scale = volume[x, rows]
                for c in range(nf):
                    target[c, x + 1, inner] = found[c + 1] * scale

        for x in ends:
            finish(x)
        start(flights[turn + 1][0])
        inner_planes(finish)
        start(flights[turn + 1][1])

    def push(step):
        ref = (push0, push1)[step]
        turn = 2 * step + 1
        across, along = flights[turn]

        def columns(group, x):
            for j in range(chunks + 2):
                rows = pl.ds(ROWS * j, ROWS)
                for k, dz in enumerate((1, -1)):
                    tile = packed[turn, group, k, rows]
                    for c in range(nf):
                        at = x * SLOT + c
                        tile = jnp.where(lane == at, rolled(ref[c, x, rows], at + (dz == 1)), tile)
                    packed[turn, group, k, rows] = tile

        def shift(group, x):
            for j in range(chunks + 2):
                rows = pl.ds(ROWS * j, ROWS)
                low, high = landed[turn, group, 0, rows], landed[turn, group, 1, rows]
                for c in range(nf):
                    at = x * SLOT + c
                    value = ref[c, x, rows]
                    shifted[0, c, x, rows] = jnp.where(lane == 0, rolled(low, nz - at), rolled(value, 1))
                    shifted[1, c, x, rows] = jnp.where(
                        lane == nz - 1, rolled(high, nz - 1 - at), rolled(value, nz - 1)
                    )

        def planes(first, count, work):
            def step(x, carry):
                work(x)
                return carry
            lax.fori_loop(first, first + count, step, 0)

        def gathered(x, j, dxs, dzs, values):
            active = act[x + 1, pl.ds(ROWS * (j + 1), ROWS)]
            for dz in dzs:
                for dx in dxs:
                    for dy in (-1, 0, 1):
                        rows = pl.ds(ROWS * (j + 1) + dy, ROWS)
                        if dz == 0:
                            terms = [ref[c, x + 1 + dx, rows] for c in range(nf)]
                        else:
                            terms = [shifted[(dz + 1) // 2, c, x + 1 + dx, rows] for c in range(nf)]
                        if (dx, dy, dz) != (0, 0, 0):
                            member = bit_of(active, dx, dy, dz)
                            terms = [jnp.where(member, v, 0.0) for v in terms]
                        values = terms if values is None else [a + b for a, b in zip(values, terms)]
            return values

        def held(x, j):
            return [total[c, x, pl.ds(ROWS * j, ROWS)] for c in range(nf)]

        def keep(x, j, values):
            for c in range(nf):
                total[c, x, pl.ds(ROWS * j, ROWS)] = values[c]

        def give(x, j, values):
            rows, inner = pl.ds(ROWS * j, ROWS), pl.ds(ROWS * (j + 1), ROWS)
            scale = inverse[x, rows]
            if step == PASSES - 1:
                for c in range(nf):
                    out[c, x, rows] = values[c] * scale
            else:
                scale = scale * pull0[0, x + 1, inner]
                for c in range(nf):
                    pull1[c, x + 1, inner] = values[c] * scale

        def add(x, dxs, dzs, first, last):
            for j in range(chunks):
                values = gathered(x, j, dxs, dzs, None if first else held(x, j))
                (give if last else keep)(x, j, values)

        arrive(along)
        planes(1, nx, lambda x: columns(0, x))
        copies = z_copies(turn, 0, ny + 2 * ROWS)
        start(copies)
        inner_planes(lambda x: add(x, (-1, 0, 1), (0,), True, False))
        for x in ends:
            add(x, own(x, -1)[0], (0,), True, False)
        arrive(copies)
        planes(1, nx, lambda x: shift(0, x))
        for x in ends:
            add(x, own(x, -1)[0], (-1, 1), False, False)
        inner_planes(lambda x: add(x, (-1, 0, 1), (-1, 1), False, True))
        arrive(across)
        for x in (0, nx + 1):
            columns(1, x)
        copies = z_copies(turn, 1, ny + 2 * ROWS)
        start(copies)
        for x in ends:
            add(x, own(x, -1)[1], (0,), False, False)
        arrive(copies)
        for x in (0, nx + 1):
            shift(1, x)
        for x in ends:
            add(x, own(x, -1)[1], (-1, 1), False, True)
        if step < PASSES - 1:
            start(flights[turn + 1][1])
            start(flights[turn + 1][0])

    for step in range(PASSES):
        pull(step)
        push(step)
    for copy in started:
        copy.wait_send()


def body(counts, fields, code, flag, bits):
    nf, nx, ny, nz = fields.shape
    frame = (nx + 2, ny + 2 * ROWS, nz)
    turns = 2 * PASSES
    vmem = pl.BlockSpec(memory_space=pltpu.VMEM)
    f32 = jnp.float32
    return pl.pallas_call(
        functools.partial(kernel, counts),
        out_shape=jax.ShapeDtypeStruct(fields.shape, f32),
        in_specs=[vmem] * 4,
        out_specs=vmem,
        scratch_shapes=[
            pltpu.VMEM((nf + 1,) + frame, f32),
            pltpu.VMEM((nf,) + frame, f32),
            pltpu.VMEM((nf,) + frame, f32),
            pltpu.VMEM((nf,) + frame, f32),
            pltpu.VMEM(frame, jnp.int32),
            pltpu.VMEM((nx, ny, nz), f32),
            pltpu.VMEM((nx, ny, nz), f32),
            pltpu.VMEM((2, nf + 1, nx, ny, nz), f32),
            pltpu.VMEM((nf + 1, nx, ny, nz), f32),
            pltpu.VMEM((2, nf) + frame, f32),
            pltpu.VMEM((turns, 2, 2, ny + 2 * ROWS, nz), f32),
            pltpu.VMEM((turns, 2, 2, ny + 2 * ROWS, nz), f32),
            pltpu.SemaphoreType.DMA((turns, len(SIDES))),
            pltpu.SemaphoreType.DMA((turns, len(SIDES))),
            pltpu.SemaphoreType.DMA((len(SIDES),)),
            pltpu.SemaphoreType.DMA((len(SIDES),)),
            pltpu.SemaphoreType.DMA((turns, 2, 2)),
            pltpu.SemaphoreType.DMA((turns, 2, 2)),
        ],
        compiler_params=pltpu.CompilerParams(collective_id=0, has_side_effects=True),
    )(fields, code, flag, bits)


def folded_kernel(
    counts, fields, code, flag, bits, out,
    raw, rawcode, bit_box, flag_box, act_box, act, pull0, push0, pull1, push1,
    edge_act, edge0, edge1, edge2, edge3, ends, act_ends,
    volume, inverse, weight, edge_volume, edge_weight,
    packed, act_packed, landed, act_landed, done,
    load_sem, x_send, x_recv, y_send, y_recv, z_send, z_recv, back_send, back_recv, token,
):
    nf, nx, ny, nz = fields.shape
    planes = 2 * nx
    half = ny // 2
    tiles = (half + 2 * REACH) // ROWS
    place = [lax.axis_index(name) for name in AXES]
    side = place[0]
    last = ny - REACH
    top, bottom = ROWS, ROWS + REACH + half

    def device(dx, dy, dz):
        step = (dx, dy, dz)
        return tuple(
            lax.rem(place[d] + step[d] + counts[d], counts[d]) if step[d] else place[d]
            for d in range(3)
        )

    def by_side(work):
        for s in (0, 1):
            @pl.when(side == s)
            def _(s=s):
                work(s)

    barrier = pltpu.get_barrier_semaphore()

    row, end_row = place[1], counts[1] - 1
    near = [(1, 0, 0), (0, 0, 1), (0, 0, -1)]
    not_first, not_last = row > 0, row < end_row

    def tell(sem, step):
        pl.semaphore_signal(sem, inc=1, device_id=device(*step), device_id_type=MESH)

    for step in near:
        tell(barrier, step)
    for there, dy in ((not_first, -1), (not_last, 1)):
        pl.when(there)(functools.partial(tell, barrier, (0, dy, 0)))

    def meet_rows():
        rising, falling, across = token.at[0], token.at[1], token.at[2]
        pl.when(row == 0)(functools.partial(tell, rising, (0, 1, 0)))
        pl.when(row == end_row)(functools.partial(tell, falling, (0, -1, 0)))
        for sem, come, go, dy in ((rising, not_first, not_last, 1), (falling, not_last, not_first, -1)):
            @pl.when(come)
            def _(sem=sem, go=go, dy=dy):
                pl.semaphore_wait(sem, 1)
                pl.when(go)(functools.partial(tell, sem, (0, dy, 0)))
        tell(across, (1, 0, 0))
        pl.semaphore_wait(across, 1)

    own_planes, far_planes = pl.ds(0, nx), pl.ds(nx, nx)

    def own_rows(s):
        if s == 0:
            return pl.ds(0, half + REACH), pl.ds(ROWS + REACH, half + REACH)
        return pl.ds(half - REACH, half + REACH), pl.ds(ROWS, half + REACH)

    def loads(s):
        box, place_in = own_rows(s)
        return [
            pltpu.make_async_copy(bits, bit_box, load_sem.at[0]),
            pltpu.make_async_copy(flag, flag_box, load_sem.at[1]),
            pltpu.make_async_copy(fields.at[:, :, box], raw.at[:, own_planes, place_in], load_sem.at[2]),
            pltpu.make_async_copy(code.at[:, box], rawcode.at[own_planes, place_in], load_sem.at[3]),
        ]

    def remote(src, dst, send, recv, step):
        return pltpu.make_async_remote_copy(
            src_ref=src, dst_ref=dst, send_sem=send, recv_sem=recv,
            device_id=device(*step), device_id_type=MESH,
        )

    def triple(from_rows, to_planes, to_rows, send, recv, step):
        return [
            remote(fields.at[:, :, from_rows], raw.at[:, to_planes, to_rows], send.at[0], recv.at[0], step),
            remote(code.at[:, from_rows], rawcode.at[to_planes, to_rows], send.at[1], recv.at[1], step),
            remote(act_box.at[:, from_rows], act.at[0, to_planes, to_rows], send.at[2], recv.at[2], step),
        ]

    def x_rows(s, t):
        if s == 0:
            size = ROWS if t < tiles - 1 else ROWS - REACH
            return pl.ds(half - REACH + ROWS * t, size), pl.ds(ROWS * (t + 1), size)
        if t == 0:
            return pl.ds(0, ROWS - REACH), pl.ds(ROWS + REACH, ROWS - REACH)
        return pl.ds(ROWS * t - REACH, ROWS), pl.ds(ROWS * (t + 1), ROWS)

    def order(s):
        return range(tiles) if s == 1 else range(tiles - 1, -1, -1)

    def x_copies(s, t):
        from_rows, to_rows = x_rows(s, t)
        return triple(from_rows, far_planes, to_rows, x_send.at[t], x_recv.at[t], (1, 0, 0))

    def y_copies(s, cross):
        low, high = pl.ds(0, REACH), pl.ds(last, REACH)
        up = (s == 0) != cross
        rows, to_rows = (high, pl.ds(top, REACH)) if up else (low, pl.ds(bottom, REACH))
        to_planes = far_planes if cross else own_planes
        step = (1 if cross else 0, 1 if up else -1, 0)
        return triple(rows, to_planes, to_rows, y_send.at[int(cross)], y_recv.at[int(cross)], step)

    def z_copies(t):
        rows = pl.ds(pl.multiple_of(ROWS * t, ROWS), ROWS)
        copies = []
        for k, dz in enumerate((1, -1)):
            copies.append(remote(
                packed.at[:, rows], landed.at[k, :, rows], z_send.at[t, k, 0], z_recv.at[t, k, 0], (0, 0, dz),
            ))
            copies.append(remote(
                act_packed.at[rows], act_landed.at[k, rows], z_send.at[t, k, 1], z_recv.at[t, k, 1], (0, 0, dz),
            ))
        return copies

    def box_rows(s, k):
        return pl.ds(pl.multiple_of(s * half + ROWS * k, ROWS), ROWS)

    def back_copy(k):
        return remote(done.at[k], out.at[:, :, box_rows(side, k)], back_send.at[k], back_recv.at[k], (1, 0, 0))

    lane = lax.broadcasted_iota(jnp.int32, (ROWS, nz), 1)
    within = jnp.bitwise_and(lane, GROUP - 1)
    member_of = jnp.right_shift(lane, GROUP.bit_length() - 1)

    def rolled(value, amount):
        amount %= nz
        return pltpu.roll(value, amount, 1) if amount else value

    def begin(s):
        copies = loads(s)
        for copy in copies:
            copy.start()
        box, place_in = own_rows(s)
        chunks = [x_copies(s, t) for t in order(1 - s)]
        pl.semaphore_wait(barrier, len(near) + not_first.astype(jnp.int32) + not_last.astype(jnp.int32))
        for copy in chunks[0][:2]:
            copy.start()
        for copy in copies[:2]:
            copy.wait()

        def plane(x, carry):
            for j in range(ny // ROWS):
                rows = pl.ds(ROWS * j, ROWS)
                act_box[x, rows] = bit_box[x, rows] * flag_box[x, rows]
            return carry

        lax.fori_loop(0, nx, plane, 0, unroll=nx)
        for copy in chunks[0][2:] + sum(chunks[1:], []):
            copy.start()

        def keep(x, carry):
            start, end, size = box.start, place_in.start, box.size
            for j in range(0, size, ROWS):
                n = min(ROWS, size - j)
                act[0, x, pl.ds(end + j, n)] = act_box[x, pl.ds(start + j, n)]
            return carry

        lax.fori_loop(0, nx, keep, 0, unroll=nx)
        for copy in copies[2:]:
            copy.wait()
        meet_rows()
        for copy in y_copies(s, False) + y_copies(s, True):
            copy.start()

    by_side(begin)

    def arrived(s, t):
        short = t == (tiles - 1) * s

        def wait_rows(size):
            rows = pl.ds(0, size)
            for copy in triple(rows, far_planes, rows, x_send.at[t], x_recv.at[t], (1, 0, 0)):
                copy.wait_recv()

        @pl.when(short)
        def _():
            wait_rows(ROWS - REACH)
            for cross in (False, True):
                for copy in y_copies(0, cross):
                    copy.wait_recv()

        @pl.when(jnp.logical_not(short))
        def _():
            wait_rows(ROWS)

    def view(ref, t, *lead):
        return ref.at[(*lead, pl.ds(pl.multiple_of(ROWS * t, ROWS), 3 * ROWS))]

    def get(ref, t, offset, *lead):
        return view(ref, t, *lead)[pl.ds(offset, ROWS)]

    def put(ref, t, offset, *lead):
        def write(value):
            view(ref, t, *lead)[pl.ds(offset, ROWS)] = value
        return write

    def strip(t):
        return pl.ds(pl.multiple_of(ROWS * t, ROWS), ROWS)

    def prepare(t):
        def plane(x, carry):
            kappa = get(rawcode, t, ROWS, x).astype(jnp.float32) * (1.0 / 1048576.0)
            put(pull0, t, ROWS, 0, x, 0)(kappa)
            for c in range(nf):
                put(pull0, t, ROWS, 0, x, c + 1)(kappa * get(raw, t, ROWS, c, x))
            others = ones_in(jnp.bitwise_and(get(act, t, ROWS, 0, x), ((1 << 27) - 1) ^ (1 << 13)))
            scale = 1.0 / (1 + others).astype(jnp.float32)
            put(inverse, t, ROWS, x)(scale)
            put(weight, t, ROWS, x)(scale * kappa)
            return carry

        lax.fori_loop(0, planes, plane, 0, unroll=planes)
        for c in range(-1, nf + 1):
            tile = None
            for x in range(planes):
                value = get(act, t, ROWS, 0, x) if c < 0 else get(pull0, t, ROWS, 0, x, c)
                value = rolled(value, GROUP * x + 2 * REACH)
                tile = value if tile is None else jnp.where(member_of == x, value, tile)
            if c < 0:
                act_packed[strip(t)] = tile
            else:
                packed[c, strip(t)] = tile
        for copy in z_copies(t):
            copy.start()

    turns = [(sx, sz) for sx in (-1, 0, 1) for sz in (-1, 0, 1)]

    def spread(tile, keep, keep_end):
        for v, (sx, sz) in enumerate(turns):
            keep(v)(rolled(tile, -(GROUP * sx + sz)))
        meet = 3 * REACH + 1
        pair = jnp.where(within == meet, rolled(tile, meet - (REACH - 1)), tile)
        for x in range(planes):
            keep_end(x, rolled(pair, -(GROUP * x + meet)))

    def beside(value, end):
        return (
            jnp.where(lane == 0, end, rolled(value, 1)),
            jnp.where(lane == nz - 1, end, rolled(value, -1)),
        )

    def unpack(t):
        for copy in z_copies(t):
            copy.wait_recv()
        at = strip(t)

        def joined(own, low, high):
            left = rolled(jnp.where(within < 2 * REACH, low, own), -REACH)
            right = rolled(jnp.where(within < 2 * REACH, own, high), REACH)
            return jnp.where(within < 2 * REACH, left, right)

        tile = joined(act_packed[at], act_landed[0, at], act_landed[1, at])

        def keep_end(x, value):
            act_ends[x] = value

        spread(tile, lambda v: put(edge_act, t, ROWS, v), keep_end)
        others = ones_in(jnp.bitwise_and(tile, ((1 << 27) - 1) ^ (1 << 13)))
        scale = 1.0 / (1 + others).astype(jnp.float32)
        for c in range(nf + 1):
            tile = joined(packed[c, at], landed[0, c, at], landed[1, c, at])
            if c == 0:
                put(edge_weight, t, ROWS)(scale * tile)

            def keep_end(x, value):
                ends[x, c] = value

            spread(tile, lambda v: put(edge0, t, ROWS, v, c), keep_end)

        def plane(x, carry):
            low, high = beside(get(act, t, ROWS, 0, x), act_ends[x])
            put(act, t, ROWS, 1, x)(low)
            put(act, t, ROWS, 2, x)(high)
            for c in range(nf + 1):
                low, high = beside(get(pull0, t, ROWS, 0, x, c), ends[x, c])
                put(pull0, t, ROWS, 1, x, c)(low)
                put(pull0, t, ROWS, 2, x, c)(high)
            return carry

        lax.fori_loop(0, planes, plane, 0, unroll=planes)

    def gathered(mask_at, value_at, arrays, pulls):
        values = list(value_at(0, 0, 0))
        center = None if pulls else mask_at(0, 0, 0)
        for sx in (-1, 0, 1):
            for sy in (-1, 0, 1):
                for sz in (-1, 0, 1):
                    if (sx, sy, sz) == (0, 0, 0):
                        continue
                    if pulls:
                        member = bit_of(mask_at(sx, sy, sz), -sx, -sy, -sz)
                    else:
                        member = bit_of(center, sx, sy, sz)
                    terms = value_at(sx, sy, sz)
                    values = [a + jnp.where(member, b, 0.0) for a, b in zip(values, terms)]
        return values

    shifts = {0: 0, -1: 1, 1: 2}

    def edge_values(source, arrays, pulls, t, first):
        def mask_at(sx, sy, sz):
            return get(edge_act, t, first + sy, turns.index((sx, sz)))

        def value_at(sx, sy, sz):
            return [get(source, t, first + sy, turns.index((sx, sz)), c) for c in range(arrays)]

        return gathered(mask_at, value_at, arrays, pulls)

    def plane_values(source, arrays, pulls, t, first, x):
        at = {0: x, -1: jnp.where(x == 0, planes - 1, x - 1), 1: jnp.where(x == planes - 1, 0, x + 1)}

        def mask_at(sx, sy, sz):
            return get(act, t, first + sy, shifts[sz], at[sx])

        def value_at(sx, sy, sz):
            return [get(source, t, first + sy, shifts[sz], at[sx], c) for c in range(arrays)]

        return gathered(mask_at, value_at, arrays, pulls)

    def finish(values, stage, read_weight, read_volume, write_volume):
        if stage == 0:
            scale = 1.0 / values[0]
            write_volume(scale)
            values = values[1:]
        elif stage == 1:
            scale = read_weight()
        else:
            scale = read_volume()
        return [value * scale for value in values]

    sources = ((pull0, edge0), (push0, edge1), (pull1, edge2), (push1, edge3))

    def advance(s, stage, t):
        first = ROWS - 1 - stage if s == 1 else ROWS + 1 + stage
        source, edge_source = sources[stage]
        target, edge_target = sources[stage + 1]
        arrays = nf + 1 if stage == 0 else nf
        pulls = stage % 2 == 0
        values = edge_values(edge_source, arrays, pulls, t, first)
        values = finish(
            values, stage, lambda: get(edge_weight, t, first),
            lambda: get(edge_volume, t, first), put(edge_volume, t, first),
        )
        for c, value in enumerate(values):
            def keep_end(x, moved):
                ends[x, c] = moved

            spread(value, lambda v: put(edge_target, t, first, v, c), keep_end)

        def plane(x, carry):
            values = plane_values(source, arrays, pulls, t, first, x)
            values = finish(
                values, stage, lambda: get(weight, t, first, x),
                lambda: get(volume, t, first, x), put(volume, t, first, x),
            )
            for c, value in enumerate(values):
                low, high = beside(value, ends[x, c])
                put(target, t, first, 0, x, c)(value)
                put(target, t, first, 1, x, c)(low)
                put(target, t, first, 2, x, c)(high)
            return carry

        lax.fori_loop(0, planes, plane, 0, unroll=planes)

    def deliver(s, t):
        k = t - s
        first = REACH if s == 1 else ROWS + REACH
        rows = box_rows(s, k)

        def result(x):
            scale = get(inverse, t, first, x)
            return [value * scale for value in plane_values(push1, nf, False, t, first, x)]

        def far(x, carry):
            for c, value in enumerate(result(nx + x)):
                done[k, c, x] = value
            return carry

        def near(x, carry):
            for c, value in enumerate(result(x)):
                out[c, x, rows] = value
            return carry

        lax.fori_loop(0, nx, far, 0, unroll=nx)
        back_copy(k).start()
        lax.fori_loop(0, nx, near, 0, unroll=nx)

    def run(s):
        def tile(u):
            return u if s == 1 else tiles - 1 - u

        def step(u, carry):
            @pl.when(u < tiles)
            def _():
                arrived(s, tile(u))
                prepare(tile(u))

            @pl.when(u > 0)
            def _():
                unpack(tile(u - 1))
                for stage in range(3):
                    advance(s, stage, tile(u - 1))

            @pl.when(u > 1)
            def _():
                deliver(s, tile(u - 1))

            return carry

        lax.fori_loop(0, tiles + 1, step, 0)

    by_side(run)

    for t in range(tiles):
        for copy in z_copies(t):
            copy.wait_send()

    def drain(s):
        for copy in y_copies(s, False) + y_copies(s, True):
            copy.wait_send()
        for t in range(tiles):
            for copy in x_copies(s, t):
                copy.wait_send()

    by_side(drain)
    for k in range(tiles - 1):
        back_copy(k).wait()


def folded_body(counts, fields, code, flag, bits):
    nf, nx, ny, nz = fields.shape
    planes = 2 * nx
    depth = ny // 2 + 2 * REACH
    tiles = depth // ROWS
    high = depth + 2 * ROWS
    f32, i32 = jnp.float32, jnp.int32
    whole = pl.BlockSpec(memory_space=pl.ANY)
    dma = pltpu.SemaphoreType.DMA

    def main(n):
        return pltpu.VMEM((3, planes, n, high, nz), f32)

    def edge(n):
        return pltpu.VMEM((9, n, high, nz), f32)

    return pl.pallas_call(
        functools.partial(folded_kernel, counts),
        out_shape=pltpu.VMEM(fields.shape, f32),
        in_specs=[whole] * 4,
        out_specs=pl.BlockSpec(memory_space=pltpu.VMEM),
        scratch_shapes=[
            pltpu.VMEM((nf, planes, high, nz), f32),
            pltpu.VMEM((planes, high, nz), i32),
            pltpu.VMEM((nx, ny, nz), i32),
            pltpu.VMEM((nx, ny, nz), i32),
            pltpu.VMEM((nx, ny, nz), i32),
            pltpu.VMEM((3, planes, high, nz), i32),
            main(nf + 1), main(nf), main(nf), main(nf),
            pltpu.VMEM((9, high, nz), i32),
            edge(nf + 1), edge(nf), edge(nf), edge(nf),
            pltpu.VMEM((planes, nf + 1, ROWS, nz), f32),
            pltpu.VMEM((planes, ROWS, nz), i32),
            pltpu.VMEM((planes, high, nz), f32),
            pltpu.VMEM((planes, high, nz), f32),
            pltpu.VMEM((planes, high, nz), f32),
            pltpu.VMEM((high, nz), f32),
            pltpu.VMEM((high, nz), f32),
            pltpu.VMEM((nf + 1, depth, nz), f32),
            pltpu.VMEM((depth, nz), i32),
            pltpu.VMEM((2, nf + 1, depth, nz), f32),
            pltpu.VMEM((2, depth, nz), i32),
            pltpu.VMEM((tiles - 1, nf, nx, ROWS, nz), f32),
            dma((4,)),
            dma((tiles, 3)), dma((tiles, 3)),
            dma((2, 3)), dma((2, 3)),
            dma((tiles, 2, 2)), dma((tiles, 2, 2)),
            dma((tiles - 1,)), dma((tiles - 1,)),
            pltpu.SemaphoreType.REGULAR((3,)),
        ],
        compiler_params=pltpu.CompilerParams(collective_id=0, has_side_effects=True),
    )(fields, code, flag, bits)


def any_body(counts, fields, code, flag, bits):
    nf, nx, ny, nz = fields.shape
    folds = (
        counts[0] == 2 and min(counts) > 1
        and 2 * nx * GROUP == nz
        and ny % (2 * ROWS) == 0 and ny // 2 >= REACH and 2 * REACH == ROWS
    )
    return (folded_body if folds else body)(counts, fields, code, flag, bits)


def solution(mesh):
    counts = tuple(mesh.shape[name] for name in AXES)
    spec = P("gx", "gy", "gz")
    whole = P(None, "gx", "gy", "gz")
    return jax.shard_map(
        functools.partial(any_body, counts),
        mesh=mesh,
        in_specs=(whole, spec, spec, spec),
        out_specs=whole,
        check_vma=False,
    )
```

```python
import functools

import jax
import jax.numpy as jnp
from jax import lax
from jax.experimental import pallas as pl
from jax.experimental.pallas import tpu as pltpu
from jax.sharding import PartitionSpec as P

PASSES = 2
MESH = pl.DeviceIdType.MESH
AXES = ("gx", "gy", "gz")
SIDES = [(dx, dy) for dx in (-1, 0, 1) for dy in (-1, 0, 1) if (dx, dy) != (0, 0)]
ROWS = 8
SLOT = 8
REACH = 2 * PASSES
GROUP = 4 * REACH


def bit_of(active, dx, dy, dz):
    index = 9 * (dx + 1) + 3 * (dy + 1) + (dz + 1)
    return jnp.bitwise_and(active, 1 << index) != 0


def ones_in(active):
    v = active - jnp.bitwise_and(jnp.right_shift(active, 1), 0x55555555)
    v = jnp.bitwise_and(v, 0x33333333) + jnp.bitwise_and(jnp.right_shift(v, 2), 0x33333333)
    v = jnp.bitwise_and(v + jnp.right_shift(v, 4), 0x0F0F0F0F)
    v = v + jnp.right_shift(v, 8)
    v = v + jnp.right_shift(v, 16)
    return jnp.bitwise_and(v, 63)


def kernel(
    counts, fields, code, flag, bits, out,
    pull0, push0, pull1, push1, act, volume, inverse, acc, total, shifted, packed, landed,
    side_send, side_recv, act_send, act_recv, z_send, z_recv,
):
    nf, nx, ny, nz = fields.shape
    place = [lax.axis_index(name) for name in AXES]

    def device(dx, dy, dz):
        step = (dx, dy, dz)
        return tuple(
            lax.rem(place[d] + step[d] + counts[d], counts[d]) if step[d] else place[d]
            for d in range(3)
        )

    barrier = pltpu.get_barrier_semaphore()
    for dx, dy in SIDES:
        pl.semaphore_signal(barrier, inc=1, device_id=device(dx, dy, 0), device_id_type=MESH)
    for dz in (-1, 1):
        pl.semaphore_signal(barrier, inc=1, device_id=device(0, 0, dz), device_id_type=MESH)

    lane = lax.broadcasted_iota(jnp.int32, (ROWS, nz), 1)
    chunks = ny // ROWS

    def loop_planes(count, work):
        def step(x, carry):
            work(x)
            return carry
        lax.fori_loop(0, count, step, 0)

    def window(side, size, first):
        if side == 0:
            return pl.ds(first, size), pl.ds(first, size)
        if side > 0:
            return pl.ds(first + size - 1, 1), pl.ds(first - 1, 1)
        return pl.ds(first, 1), pl.ds(first + size, 1)

    def side_copies(ref, lead, send, recv):
        copies = []
        for k, (dx, dy) in enumerate(SIDES):
            from_x, to_x = window(dx, nx, 1)
            from_y, to_y = window(dy, ny, ROWS)
            copies.append(
                pltpu.make_async_remote_copy(
                    src_ref=ref.at[lead + (from_x, from_y)],
                    dst_ref=ref.at[lead + (to_x, to_y)],
                    send_sem=send(k),
                    recv_sem=recv(k),
                    device_id=device(dx, dy, 0),
                    device_id_type=MESH,
                )
            )
        return copies

    def z_copies(turn, group, rows):
        copies = []
        for k, dz in enumerate((1, -1)):
            copies.append(
                pltpu.make_async_remote_copy(
                    src_ref=packed.at[turn, group, k, pl.ds(0, rows)],
                    dst_ref=landed.at[turn, group, k, pl.ds(0, rows)],
                    send_sem=z_send.at[turn, group, k],
                    recv_sem=z_recv.at[turn, group, k],
                    device_id=device(0, 0, dz),
                    device_id_type=MESH,
                )
            )
        return copies

    started = []

    def start(copies):
        for copy in copies:
            copy.start()
        started.extend(copies)

    def arrive(copies):
        for copy in copies:
            copy.wait_recv()

    def turn_copies(turn):
        ref = (pull0, push0, pull1, push1)[turn]
        copies = side_copies(
            ref, (slice(None),), lambda k: side_send.at[turn, k], lambda k: side_recv.at[turn, k]
        )
        sides = SIDES
        if turn == 0:
            copies += side_copies(act, (), lambda k: act_send.at[k], lambda k: act_recv.at[k])
            sides = SIDES + SIDES
        across = [copy for copy, side in zip(copies, sides) if side[0] != 0]
        along = [copy for copy, side in zip(copies, sides) if side[0] == 0]
        return across, along

    ends = sorted({0, nx - 1})

    def inner_planes(work):
        if nx > 2:
            def step(x, carry):
                work(x)
                return carry
            lax.fori_loop(1, nx - 1, step, 0)

    def own(x, sign):
        inside = [dx for dx in (-1, 0, 1) if 0 <= x - sign * dx < nx]
        return inside, [dx for dx in (-1, 0, 1) if dx not in inside]

    def rolled(value, amount):
        return pltpu.roll(value, amount % nz, 1)

    def prepare(x):
        for j in range(chunks):
            rows, inner = pl.ds(ROWS * j, ROWS), pl.ds(ROWS * (j + 1), ROWS)
            kappa = code[x, rows].astype(jnp.float32) * (1.0 / 1048576.0)
            active = bits[x, rows] * flag[x, rows]
            act[x + 1, inner] = active
            pull0[0, x + 1, inner] = kappa
            for c in range(nf):
                pull0[c + 1, x + 1, inner] = kappa * fields[c, x, rows]
            others = ones_in(jnp.bitwise_and(active, ((1 << 27) - 1) ^ (1 << 13)))
            inverse[x, rows] = 1.0 / (1 + others).astype(jnp.float32)

    loop_planes(nx, prepare)
    packed[...] = jnp.zeros_like(packed)
    pl.semaphore_wait(barrier, len(SIDES) + 2)
    flights = [turn_copies(turn) for turn in range(2 * PASSES)]
    start(flights[0][1])
    start(flights[0][0])

    def pull(step):
        ref = (pull0, pull1)[step]
        target = (push0, push1)[step]
        arrays = range(nf + 1) if step == 0 else range(1, nf + 1)
        turn = 2 * step
        base = 0 if step == 0 else 1
        across, along = flights[turn]

        def sums(x, j, dxs, dzs, found):
            for dx in dxs:
                for dy in (-1, 0, 1):
                    rows = pl.ds(ROWS * (j + 1) - dy, ROWS)
                    active = act[x + 1 - dx, rows]
                    values = [ref[c - base, x + 1 - dx, rows] for c in arrays]
                    for dz in dzs:
                        if (dx, dy, dz) == (0, 0, 0):
                            terms = values
                        else:
                            member = bit_of(active, dx, dy, dz)
                            terms = [jnp.where(member, v, 0.0) for v in values]
                        if dz in found:
                            found[dz] = [a + b for a, b in zip(found[dz], terms)]
                        else:
                            found[dz] = terms
            return found

        def pack(x, j, found):
            rows = pl.ds(ROWS * j, ROWS)
            for k, dz in enumerate((1, -1)):
                tile = packed[turn, 0, k, rows]
                for c, value in zip(arrays, found[dz]):
                    acc[k, c, x, rows] = value
                    at = x * SLOT + c
                    tile = jnp.where(lane == at, rolled(value, at + (dz == 1)), tile)
                packed[turn, 0, k, rows] = tile

        def early(x, dxs, complete):
            for j in range(chunks):
                rows = pl.ds(ROWS * j, ROWS)
                found = sums(x, j, dxs, (1, 0, -1), {})
                for c, value in zip(arrays, found[0]):
                    total[c, x, rows] = value
                if complete:
                    pack(x, j, found)
                else:
                    for k, dz in enumerate((1, -1)):
                        for c, value in zip(arrays, found[dz]):
                            acc[k, c, x, rows] = value

        arrive(along)
        inner_planes(lambda x: early(x, (-1, 0, 1), True))
        for x in ends:
            early(x, own(x, 1)[0], False)
        arrive(across)
        for x in ends:
            for j in range(chunks):
                rows = pl.ds(ROWS * j, ROWS)
                found = {dz: [acc[k, c, x, rows] for c in arrays] for k, dz in enumerate((1, -1))}
                pack(x, j, sums(x, j, own(x, 1)[1], (1, -1), found))
        copies = z_copies(turn, 0, ny)
        start(copies)
        for x in ends:
            for j in range(chunks):
                rows = pl.ds(ROWS * j, ROWS)
                found = {0: [total[c, x, rows] for c in arrays]}
                for c, value in zip(arrays, sums(x, j, own(x, 1)[1], (0,), found)[0]):
                    total[c, x, rows] = value
        arrive(copies)

        def finish(x):
            for j in range(chunks):
                rows, inner = pl.ds(ROWS * j, ROWS), pl.ds(ROWS * (j + 1), ROWS)
                low, high = landed[turn, 0, 0, rows], landed[turn, 0, 1, rows]
                found = {}
                for c in arrays:
                    at = x * SLOT + c
                    from_low = jnp.where(lane == 0, rolled(low, nz - at), rolled(acc[0, c, x, rows], 1))
                    from_high = jnp.where(
                        lane == nz - 1, rolled(high, nz - 1 - at), rolled(acc[1, c, x, rows], nz - 1)
                    )
                    found[c] = total[c, x, rows] + from_low + from_high
                if step == 0:
                    scale = 1.0 / found[0]
                    volume[x, rows] = scale
                else:
                    scale = volume[x, rows]
                for c in range(nf):
                    target[c, x + 1, inner] = found[c + 1] * scale

        for x in ends:
            finish(x)
        start(flights[turn + 1][0])
        inner_planes(finish)
        start(flights[turn + 1][1])

    def push(step):
        ref = (push0, push1)[step]
        turn = 2 * step + 1
        across, along = flights[turn]

        def columns(group, x):
            for j in range(chunks + 2):
                rows = pl.ds(ROWS * j, ROWS)
                for k, dz in enumerate((1, -1)):
                    tile = packed[turn, group, k, rows]
                    for c in range(nf):
                        at = x * SLOT + c
                        tile = jnp.where(lane == at, rolled(ref[c, x, rows], at + (dz == 1)), tile)
                    packed[turn, group, k, rows] = tile

        def shift(group, x):
            for j in range(chunks + 2):
                rows = pl.ds(ROWS * j, ROWS)
                low, high = landed[turn, group, 0, rows], landed[turn, group, 1, rows]
                for c in range(nf):
                    at = x * SLOT + c
                    value = ref[c, x, rows]
                    shifted[0, c, x, rows] = jnp.where(lane == 0, rolled(low, nz - at), rolled(value, 1))
                    shifted[1, c, x, rows] = jnp.where(
                        lane == nz - 1, rolled(high, nz - 1 - at), rolled(value, nz - 1)
                    )

        def planes(first, count, work):
            def step(x, carry):
                work(x)
                return carry
            lax.fori_loop(first, first + count, step, 0)

        def gathered(x, j, dxs, dzs, values):
            active = act[x + 1, pl.ds(ROWS * (j + 1), ROWS)]
            for dz in dzs:
                for dx in dxs:
                    for dy in (-1, 0, 1):
                        rows = pl.ds(ROWS * (j + 1) + dy, ROWS)
                        if dz == 0:
                            terms = [ref[c, x + 1 + dx, rows] for c in range(nf)]
                        else:
                            terms = [shifted[(dz + 1) // 2, c, x + 1 + dx, rows] for c in range(nf)]
                        if (dx, dy, dz) != (0, 0, 0):
                            member = bit_of(active, dx, dy, dz)
                            terms = [jnp.where(member, v, 0.0) for v in terms]
                        values = terms if values is None else [a + b for a, b in zip(values, terms)]
            return values

        def held(x, j):
            return [total[c, x, pl.ds(ROWS * j, ROWS)] for c in range(nf)]

        def keep(x, j, values):
            for c in range(nf):
                total[c, x, pl.ds(ROWS * j, ROWS)] = values[c]

        def give(x, j, values):
            rows, inner = pl.ds(ROWS * j, ROWS), pl.ds(ROWS * (j + 1), ROWS)
            scale = inverse[x, rows]
            if step == PASSES - 1:
                for c in range(nf):
                    out[c, x, rows] = values[c] * scale
            else:
                scale = scale * pull0[0, x + 1, inner]
                for c in range(nf):
                    pull1[c, x + 1, inner] = values[c] * scale

        def add(x, dxs, dzs, first, last):
            for j in range(chunks):
                values = gathered(x, j, dxs, dzs, None if first else held(x, j))
                (give if last else keep)(x, j, values)

        arrive(along)
        planes(1, nx, lambda x: columns(0, x))
        copies = z_copies(turn, 0, ny + 2 * ROWS)
        start(copies)
        inner_planes(lambda x: add(x, (-1, 0, 1), (0,), True, False))
        for x in ends:
            add(x, own(x, -1)[0], (0,), True, False)
        arrive(copies)
        planes(1, nx, lambda x: shift(0, x))
        for x in ends:
            add(x, own(x, -1)[0], (-1, 1), False, False)
        inner_planes(lambda x: add(x, (-1, 0, 1), (-1, 1), False, True))
        arrive(across)
        for x in (0, nx + 1):
            columns(1, x)
        copies = z_copies(turn, 1, ny + 2 * ROWS)
        start(copies)
        for x in ends:
            add(x, own(x, -1)[1], (0,), False, False)
        arrive(copies)
        for x in (0, nx + 1):
            shift(1, x)
        for x in ends:
            add(x, own(x, -1)[1], (-1, 1), False, True)
        if step < PASSES - 1:
            start(flights[turn + 1][1])
            start(flights[turn + 1][0])

    for step in range(PASSES):
        pull(step)
        push(step)
    for copy in started:
        copy.wait_send()


def body(counts, fields, code, flag, bits):
    nf, nx, ny, nz = fields.shape
    frame = (nx + 2, ny + 2 * ROWS, nz)
    turns = 2 * PASSES
    vmem = pl.BlockSpec(memory_space=pltpu.VMEM)
    f32 = jnp.float32
    return pl.pallas_call(
        functools.partial(kernel, counts),
        out_shape=jax.ShapeDtypeStruct(fields.shape, f32),
        in_specs=[vmem] * 4,
        out_specs=vmem,
        scratch_shapes=[
            pltpu.VMEM((nf + 1,) + frame, f32),
            pltpu.VMEM((nf,) + frame, f32),
            pltpu.VMEM((nf,) + frame, f32),
            pltpu.VMEM((nf,) + frame, f32),
            pltpu.VMEM(frame, jnp.int32),
            pltpu.VMEM((nx, ny, nz), f32),
            pltpu.VMEM((nx, ny, nz), f32),
            pltpu.VMEM((2, nf + 1, nx, ny, nz), f32),
            pltpu.VMEM((nf + 1, nx, ny, nz), f32),
            pltpu.VMEM((2, nf) + frame, f32),
            pltpu.VMEM((turns, 2, 2, ny + 2 * ROWS, nz), f32),
            pltpu.VMEM((turns, 2, 2, ny + 2 * ROWS, nz), f32),
            pltpu.SemaphoreType.DMA((turns, len(SIDES))),
            pltpu.SemaphoreType.DMA((turns, len(SIDES))),
            pltpu.SemaphoreType.DMA((len(SIDES),)),
            pltpu.SemaphoreType.DMA((len(SIDES),)),
            pltpu.SemaphoreType.DMA((turns, 2, 2)),
            pltpu.SemaphoreType.DMA((turns, 2, 2)),
        ],
        compiler_params=pltpu.CompilerParams(collective_id=0, has_side_effects=True),
    )(fields, code, flag, bits)


def folded_kernel(
    counts, fields, code, flag, bits, out,
    field_box, code_box, raw, rawcode, bit_box, flag_box, act_box, act, pull0, push0, pull1, push1,
    edge_act, edge0, edge1, edge2, edge3, ends, act_ends,
    volume, inverse, weight, edge_volume, edge_weight,
    packed, act_packed, landed, act_landed, done,
    load_sem, x_send, x_recv, y_send, y_recv, z_send, z_recv, back_send, back_recv, token,
):
    nf, nx, ny, nz = fields.shape
    planes = 2 * nx
    half = ny // 2
    tiles = (half + 2 * REACH) // ROWS
    place = [lax.axis_index(name) for name in AXES]
    side = place[0]
    last = ny - REACH
    top, bottom = ROWS, ROWS + REACH + half

    def device(dx, dy, dz):
        step = (dx, dy, dz)
        return tuple(
            lax.rem(place[d] + step[d] + counts[d], counts[d]) if step[d] else place[d]
            for d in range(3)
        )

    def by_side(work):
        for s in (0, 1):
            @pl.when(side == s)
            def _(s=s):
                work(s)

    barrier = pltpu.get_barrier_semaphore()

    row, end_row = place[1], counts[1] - 1
    near = [(1, 0, 0), (0, 0, 1), (0, 0, -1)]
    not_first, not_last = row > 0, row < end_row

    def tell(sem, step):
        pl.semaphore_signal(sem, inc=1, device_id=device(*step), device_id_type=MESH)

    for step in near:
        tell(barrier, step)
    for there, dy in ((not_first, -1), (not_last, 1)):
        pl.when(there)(functools.partial(tell, barrier, (0, dy, 0)))

    rising, falling, across = token.at[0], token.at[1], token.at[2]

    def pass_tokens(hop):
        for sem, first, dy in ((rising, 0, 1), (falling, end_row, -1)):
            @pl.when(row == first + dy * hop)
            def _(sem=sem, dy=dy):
                if hop > 0:
                    pl.semaphore_wait(sem, 1)
                if hop < counts[1] - 1:
                    tell(sem, (0, dy, 0))

    own_planes, far_planes = pl.ds(0, nx), pl.ds(nx, nx)

    def own_rows(s):
        if s == 0:
            return pl.ds(0, half + REACH), pl.ds(ROWS + REACH, half + REACH)
        return pl.ds(half - REACH, half + REACH), pl.ds(ROWS, half + REACH)

    def loads(s):
        box, place_in = own_rows(s)
        return [
            pltpu.make_async_copy(fields, field_box, load_sem.at[4]),
            pltpu.make_async_copy(code, code_box, load_sem.at[5]),
            pltpu.make_async_copy(bits, bit_box, load_sem.at[0]),
            pltpu.make_async_copy(flag, flag_box, load_sem.at[1]),
            pltpu.make_async_copy(fields.at[:, :, box], raw.at[:, own_planes, place_in], load_sem.at[2]),
            pltpu.make_async_copy(code.at[:, box], rawcode.at[own_planes, place_in], load_sem.at[3]),
        ]

    def remote(src, dst, send, recv, step):
        return pltpu.make_async_remote_copy(
            src_ref=src, dst_ref=dst, send_sem=send, recv_sem=recv,
            device_id=device(*step), device_id_type=MESH,
        )

    def triple(from_rows, to_planes, to_rows, send, recv, step):
        return [
            remote(field_box.at[:, :, from_rows], raw.at[:, to_planes, to_rows], send.at[0], recv.at[0], step),
            remote(code_box.at[:, from_rows], rawcode.at[to_planes, to_rows], send.at[1], recv.at[1], step),
            remote(act_box.at[:, from_rows], act.at[0, to_planes, to_rows], send.at[2], recv.at[2], step),
        ]

    def x_rows(s, t):
        if s == 0:
            size = ROWS if t < tiles - 1 else ROWS - REACH
            return pl.ds(half - REACH + ROWS * t, size), pl.ds(ROWS * (t + 1), size)
        if t == 0:
            return pl.ds(0, ROWS - REACH), pl.ds(ROWS + REACH, ROWS - REACH)
        return pl.ds(ROWS * t - REACH, ROWS), pl.ds(ROWS * (t + 1), ROWS)

    def order(s):
        return range(tiles) if s == 1 else range(tiles - 1, -1, -1)

    def x_copies(s, t):
        from_rows, to_rows = x_rows(s, t)
        return triple(from_rows, far_planes, to_rows, x_send.at[t], x_recv.at[t], (1, 0, 0))

    def y_copies(s, cross):
        low, high = pl.ds(0, REACH), pl.ds(last, REACH)
        up = (s == 0) != cross
        rows, to_rows = (high, pl.ds(top, REACH)) if up else (low, pl.ds(bottom, REACH))
        to_planes = far_planes if cross else own_planes
        step = (1 if cross else 0, 1 if up else -1, 0)
        return triple(rows, to_planes, to_rows, y_send.at[int(cross)], y_recv.at[int(cross)], step)

    def z_copies(t):
        rows = pl.ds(pl.multiple_of(ROWS * t, ROWS), ROWS)
        copies = []
        for k, dz in enumerate((1, -1)):
            copies.append(remote(
                packed.at[:, rows], landed.at[k, :, rows], z_send.at[t, k, 0], z_recv.at[t, k, 0], (0, 0, dz),
            ))
            copies.append(remote(
                act_packed.at[rows], act_landed.at[k, rows], z_send.at[t, k, 1], z_recv.at[t, k, 1], (0, 0, dz),
            ))
        return copies

    def box_rows(s, k):
        return pl.ds(pl.multiple_of(s * half + ROWS * k, ROWS), ROWS)

    parts = [(first, size) for first, size in ((0, nx // 2), (nx // 2, nx - nx // 2)) if size]

    def back_copy(k, part):
        some = pl.ds(*parts[part])
        return remote(
            done.at[k, :, some], out.at[:, some, box_rows(side, k)], back_send.at[k, part], back_recv.at[k, part], (1, 0, 0),
        )

    lane = lax.broadcasted_iota(jnp.int32, (ROWS, nz), 1)
    within = jnp.bitwise_and(lane, GROUP - 1)
    member_of = jnp.right_shift(lane, GROUP.bit_length() - 1)

    def rolled(value, amount):
        amount %= nz
        return pltpu.roll(value, amount, 1) if amount else value

    def begin(s):
        copies = loads(s)
        for copy in copies:
            copy.start()
        box, place_in = own_rows(s)
        chunks = [x_copies(s, t) for t in order(1 - s)]
        pl.semaphore_wait(barrier, len(near) + not_first.astype(jnp.int32) + not_last.astype(jnp.int32))
        for copy in copies[:2]:
            copy.wait()
        for copy in chunks[0][:2]:
            copy.start()
        for copy in copies[2:4]:
            copy.wait()

        def plane(x, carry):
            for j in range(ny // ROWS):
                rows = pl.ds(ROWS * j, ROWS)
                act_box[x, rows] = bit_box[x, rows] * flag_box[x, rows]
            return carry

        lax.fori_loop(0, nx, plane, 0, unroll=nx)
        for copy in chunks[0][2:] + sum(chunks[1:], []):
            copy.start()

        for hop in range(counts[1] - 1):
            pass_tokens(hop)

        def keep(x, carry):
            start, end, size = box.start, place_in.start, box.size
            for j in range(0, size, ROWS):
                n = min(ROWS, size - j)
                act[0, x, pl.ds(end + j, n)] = act_box[x, pl.ds(start + j, n)]
            return carry

        lax.fori_loop(0, nx, keep, 0, unroll=nx)
        for copy in copies[4:]:
            copy.wait()

    by_side(begin)

    def arrived(s, t):
        short = t == (tiles - 1) * s

        def wait_rows(size):
            rows = pl.ds(0, size)
            for copy in triple(rows, far_planes, rows, x_send.at[t], x_recv.at[t], (1, 0, 0)):
                copy.wait_recv()

        @pl.when(short)
        def _():
            wait_rows(ROWS - REACH)
            for cross in (False, True):
                for copy in y_copies(0, cross):
                    copy.wait_recv()

        @pl.when(jnp.logical_not(short))
        def _():
            wait_rows(ROWS)

    def view(ref, t, *lead):
        return ref.at[(*lead, pl.ds(pl.multiple_of(ROWS * t, ROWS), 3 * ROWS))]

    def get(ref, t, offset, *lead):
        return view(ref, t, *lead)[pl.ds(offset, ROWS)]

    def put(ref, t, offset, *lead):
        def write(value):
            view(ref, t, *lead)[pl.ds(offset, ROWS)] = value
        return write

    def strip(t):
        return pl.ds(pl.multiple_of(ROWS * t, ROWS), ROWS)

    def prepare(t):
        def plane(x, carry):
            kappa = get(rawcode, t, ROWS, x).astype(jnp.float32) * (1.0 / 1048576.0)
            put(pull0, t, ROWS, 0, x, 0)(kappa)
            for c in range(nf):
                put(pull0, t, ROWS, 0, x, c + 1)(kappa * get(raw, t, ROWS, c, x))
            others = ones_in(jnp.bitwise_and(get(act, t, ROWS, 0, x), ((1 << 27) - 1) ^ (1 << 13)))
            scale = 1.0 / (1 + others).astype(jnp.float32)
            put(inverse, t, ROWS, x)(scale)
            put(weight, t, ROWS, x)(scale * kappa)
            return carry

        lax.fori_loop(0, planes, plane, 0, unroll=planes)
        for c in range(-1, nf + 1):
            tile = None
            for x in range(planes):
                value = get(act, t, ROWS, 0, x) if c < 0 else get(pull0, t, ROWS, 0, x, c)
                value = rolled(value, GROUP * x + 2 * REACH)
                tile = value if tile is None else jnp.where(member_of == x, value, tile)
            if c < 0:
                act_packed[strip(t)] = tile
            else:
                packed[c, strip(t)] = tile
        for copy in z_copies(t):
            copy.start()

    turns = [(sx, sz) for sx in (-1, 0, 1) for sz in (-1, 0, 1)]

    def spread(tile, keep, keep_end):
        for v, (sx, sz) in enumerate(turns):
            keep(v)(rolled(tile, -(GROUP * sx + sz)))
        meet = 3 * REACH + 1
        pair = jnp.where(within == meet, rolled(tile, meet - (REACH - 1)), tile)
        for x in range(planes):
            keep_end(x, rolled(pair, -(GROUP * x + meet)))

    def beside(value, end):
        return (
            jnp.where(lane == 0, end, rolled(value, 1)),
            jnp.where(lane == nz - 1, end, rolled(value, -1)),
        )

    def unpack(t):
        for copy in z_copies(t):
            copy.wait_recv()
        at = strip(t)

        def joined(own, low, high):
            left = rolled(jnp.where(within < 2 * REACH, low, own), -REACH)
            right = rolled(jnp.where(within < 2 * REACH, own, high), REACH)
            return jnp.where(within < 2 * REACH, left, right)

        tile = joined(act_packed[at], act_landed[0, at], act_landed[1, at])

        def keep_end(x, value):
            act_ends[x] = value

        spread(tile, lambda v: put(edge_act, t, ROWS, v), keep_end)
        others = ones_in(jnp.bitwise_and(tile, ((1 << 27) - 1) ^ (1 << 13)))
        scale = 1.0 / (1 + others).astype(jnp.float32)
        for c in range(nf + 1):
            tile = joined(packed[c, at], landed[0, c, at], landed[1, c, at])
            if c == 0:
                put(edge_weight, t, ROWS)(scale * tile)

            def keep_end(x, value):
                ends[x, c] = value

            spread(tile, lambda v: put(edge0, t, ROWS, v, c), keep_end)

        def plane(x, carry):
            low, high = beside(get(act, t, ROWS, 0, x), act_ends[x])
            put(act, t, ROWS, 1, x)(low)
            put(act, t, ROWS, 2, x)(high)
            for c in range(nf + 1):
                low, high = beside(get(pull0, t, ROWS, 0, x, c), ends[x, c])
                put(pull0, t, ROWS, 1, x, c)(low)
                put(pull0, t, ROWS, 2, x, c)(high)
            return carry

        lax.fori_loop(0, planes, plane, 0, unroll=planes)

    def gathered(mask_at, value_at, arrays, pulls):
        values = list(value_at(0, 0, 0))
        center = None if pulls else mask_at(0, 0, 0)
        for sx in (-1, 0, 1):
            for sy in (-1, 0, 1):
                for sz in (-1, 0, 1):
                    if (sx, sy, sz) == (0, 0, 0):
                        continue
                    if pulls:
                        member = bit_of(mask_at(sx, sy, sz), -sx, -sy, -sz)
                    else:
                        member = bit_of(center, sx, sy, sz)
                    terms = value_at(sx, sy, sz)
                    values = [a + jnp.where(member, b, 0.0) for a, b in zip(values, terms)]
        return values

    shifts = {0: 0, -1: 1, 1: 2}

    def edge_values(source, arrays, pulls, t, first):
        def mask_at(sx, sy, sz):
            return get(edge_act, t, first + sy, turns.index((sx, sz)))

        def value_at(sx, sy, sz):
            return [get(source, t, first + sy, turns.index((sx, sz)), c) for c in range(arrays)]

        return gathered(mask_at, value_at, arrays, pulls)

    def plane_values(source, arrays, pulls, t, first, x):
        at = {0: x, -1: jnp.where(x == 0, planes - 1, x - 1), 1: jnp.where(x == planes - 1, 0, x + 1)}

        def mask_at(sx, sy, sz):
            return get(act, t, first + sy, shifts[sz], at[sx])

        def value_at(sx, sy, sz):
            return [get(source, t, first + sy, shifts[sz], at[sx], c) for c in range(arrays)]

        return gathered(mask_at, value_at, arrays, pulls)

    def finish(values, stage, read_weight, read_volume, write_volume):
        if stage == 0:
            scale = 1.0 / values[0]
            write_volume(scale)
            values = values[1:]
        elif stage == 1:
            scale = read_weight()
        else:
            scale = read_volume()
        return [value * scale for value in values]

    sources = ((pull0, edge0), (push0, edge1), (pull1, edge2), (push1, edge3))

    def advance(s, stage, t):
        first = ROWS - 1 - stage if s == 1 else ROWS + 1 + stage
        source, edge_source = sources[stage]
        target, edge_target = sources[stage + 1]
        arrays = nf + 1 if stage == 0 else nf
        pulls = stage % 2 == 0
        values = edge_values(edge_source, arrays, pulls, t, first)
        values = finish(
            values, stage, lambda: get(edge_weight, t, first),
            lambda: get(edge_volume, t, first), put(edge_volume, t, first),
        )
        for c, value in enumerate(values):
            def keep_end(x, moved):
                ends[x, c] = moved

            spread(value, lambda v: put(edge_target, t, first, v, c), keep_end)

        def plane(x, carry):
            values = plane_values(source, arrays, pulls, t, first, x)
            values = finish(
                values, stage, lambda: get(weight, t, first, x),
                lambda: get(volume, t, first, x), put(volume, t, first, x),
            )
            for c, value in enumerate(values):
                low, high = beside(value, ends[x, c])
                put(target, t, first, 0, x, c)(value)
                put(target, t, first, 1, x, c)(low)
                put(target, t, first, 2, x, c)(high)
            return carry

        lax.fori_loop(0, planes, plane, 0, unroll=planes)

    def deliver(s, t):
        k = t - s
        first = REACH if s == 1 else ROWS + REACH
        rows = box_rows(s, k)

        def result(x):
            scale = get(inverse, t, first, x)
            return [value * scale for value in plane_values(push1, nf, False, t, first, x)]

        def far(x, carry):
            for c, value in enumerate(result(nx + x)):
                done[k, c, x] = value
            return carry

        def near(x, carry):
            for c, value in enumerate(result(x)):
                out[c, x, rows] = value
            return carry

        for part, (start, size) in enumerate(parts):
            lax.fori_loop(start, start + size, far, 0, unroll=size)
            back_copy(k, part).start()
        lax.fori_loop(0, nx, near, 0, unroll=nx)

    def run(s):
        def tile(u):
            return u if s == 1 else tiles - 1 - u

        def step(u, carry):
            @pl.when(u < tiles)
            def _():
                arrived(s, tile(u))
                prepare(tile(u))

            @pl.when(u == 0)
            def _():
                pass_tokens(counts[1] - 1)
                tell(across, (1, 0, 0))

            @pl.when(u == 1)
            def _():
                pl.semaphore_wait(across, 1)
                for copy in y_copies(s, False) + y_copies(s, True):
                    copy.start()

            @pl.when(u > 0)
            def _():
                unpack(tile(u - 1))
                for stage in range(3):
                    advance(s, stage, tile(u - 1))

            @pl.when(u > 1)
            def _():
                deliver(s, tile(u - 1))

            return carry

        lax.fori_loop(0, tiles + 1, step, 0)

    by_side(run)

    for t in range(tiles):
        for copy in z_copies(t):
            copy.wait_send()

    def drain(s):
        for copy in y_copies(s, False) + y_copies(s, True):
            copy.wait_send()
        for t in range(tiles):
            for copy in x_copies(s, t):
                copy.wait_send()

    by_side(drain)
    for k in range(tiles - 1):
        for part in range(len(parts)):
            back_copy(k, part).wait()


def folded_body(counts, fields, code, flag, bits):
    nf, nx, ny, nz = fields.shape
    planes = 2 * nx
    depth = ny // 2 + 2 * REACH
    tiles = depth // ROWS
    high = depth + 2 * ROWS
    f32, i32 = jnp.float32, jnp.int32
    whole = pl.BlockSpec(memory_space=pl.ANY)
    dma = pltpu.SemaphoreType.DMA

    def main(n):
        return pltpu.VMEM((3, planes, n, high, nz), f32)

    def edge(n):
        return pltpu.VMEM((9, n, high, nz), f32)

    return pl.pallas_call(
        functools.partial(folded_kernel, counts),
        out_shape=pltpu.VMEM(fields.shape, f32),
        in_specs=[whole] * 4,
        out_specs=pl.BlockSpec(memory_space=pltpu.VMEM),
        scratch_shapes=[
            pltpu.VMEM((nf, nx, ny, nz), f32),
            pltpu.VMEM((nx, ny, nz), i32),
            pltpu.VMEM((nf, planes, high, nz), f32),
            pltpu.VMEM((planes, high, nz), i32),
            pltpu.VMEM((nx, ny, nz), i32),
            pltpu.VMEM((nx, ny, nz), i32),
            pltpu.VMEM((nx, ny, nz), i32),
            pltpu.VMEM((3, planes, high, nz), i32),
            main(nf + 1), main(nf), main(nf), main(nf),
            pltpu.VMEM((9, high, nz), i32),
            edge(nf + 1), edge(nf), edge(nf), edge(nf),
            pltpu.VMEM((planes, nf + 1, ROWS, nz), f32),
            pltpu.VMEM((planes, ROWS, nz), i32),
            pltpu.VMEM((planes, high, nz), f32),
            pltpu.VMEM((planes, high, nz), f32),
            pltpu.VMEM((planes, high, nz), f32),
            pltpu.VMEM((high, nz), f32),
            pltpu.VMEM((high, nz), f32),
            pltpu.VMEM((nf + 1, depth, nz), f32),
            pltpu.VMEM((depth, nz), i32),
            pltpu.VMEM((2, nf + 1, depth, nz), f32),
            pltpu.VMEM((2, depth, nz), i32),
            pltpu.VMEM((tiles - 1, nf, nx, ROWS, nz), f32),
            dma((6,)),
            dma((tiles, 3)), dma((tiles, 3)),
            dma((2, 3)), dma((2, 3)),
            dma((tiles, 2, 2)), dma((tiles, 2, 2)),
            dma((tiles - 1, 2)), dma((tiles - 1, 2)),
            pltpu.SemaphoreType.REGULAR((3,)),
        ],
        compiler_params=pltpu.CompilerParams(collective_id=0, has_side_effects=True),
    )(fields, code, flag, bits)


def any_body(counts, fields, code, flag, bits):
    nf, nx, ny, nz = fields.shape
    folds = (
        counts[0] == 2 and min(counts) > 1
        and 2 * nx * GROUP == nz
        and ny % (2 * ROWS) == 0 and ny // 2 >= REACH and 2 * REACH == ROWS
    )
    return (folded_body if folds else body)(counts, fields, code, flag, bits)


def solution(mesh):
    counts = tuple(mesh.shape[name] for name in AXES)
    spec = P("gx", "gy", "gz")
    whole = P(None, "gx", "gy", "gz")
    return jax.shard_map(
        functools.partial(any_body, counts),
        mesh=mesh,
        in_specs=(whole, spec, spec, spec),
        out_specs=whole,
        check_vma=False,
    )
```

```python
import functools

import jax
import jax.numpy as jnp
from jax import lax
from jax.experimental import pallas as pl
from jax.experimental.pallas import tpu as pltpu
from jax.sharding import PartitionSpec as P

PASSES = 2
MESH = pl.DeviceIdType.MESH
AXES = ("gx", "gy", "gz")
SIDES = [(dx, dy) for dx in (-1, 0, 1) for dy in (-1, 0, 1) if (dx, dy) != (0, 0)]
ROWS = 8
SLOT = 8
REACH = 2 * PASSES
GROUP = 4 * REACH


def bit_of(active, dx, dy, dz):
    index = 9 * (dx + 1) + 3 * (dy + 1) + (dz + 1)
    return jnp.bitwise_and(active, 1 << index) != 0


def ones_in(active):
    v = active - jnp.bitwise_and(jnp.right_shift(active, 1), 0x55555555)
    v = jnp.bitwise_and(v, 0x33333333) + jnp.bitwise_and(jnp.right_shift(v, 2), 0x33333333)
    v = jnp.bitwise_and(v + jnp.right_shift(v, 4), 0x0F0F0F0F)
    v = v + jnp.right_shift(v, 8)
    v = v + jnp.right_shift(v, 16)
    return jnp.bitwise_and(v, 63)


def kernel(
    counts, fields, code, flag, bits, out,
    pull0, push0, pull1, push1, act, volume, inverse, acc, total, shifted, packed, landed,
    side_send, side_recv, act_send, act_recv, z_send, z_recv,
):
    nf, nx, ny, nz = fields.shape
    place = [lax.axis_index(name) for name in AXES]

    def device(dx, dy, dz):
        step = (dx, dy, dz)
        return tuple(
            lax.rem(place[d] + step[d] + counts[d], counts[d]) if step[d] else place[d]
            for d in range(3)
        )

    barrier = pltpu.get_barrier_semaphore()
    for dx, dy in SIDES:
        pl.semaphore_signal(barrier, inc=1, device_id=device(dx, dy, 0), device_id_type=MESH)
    for dz in (-1, 1):
        pl.semaphore_signal(barrier, inc=1, device_id=device(0, 0, dz), device_id_type=MESH)

    lane = lax.broadcasted_iota(jnp.int32, (ROWS, nz), 1)
    chunks = ny // ROWS

    def loop_planes(count, work):
        def step(x, carry):
            work(x)
            return carry
        lax.fori_loop(0, count, step, 0)

    def window(side, size, first):
        if side == 0:
            return pl.ds(first, size), pl.ds(first, size)
        if side > 0:
            return pl.ds(first + size - 1, 1), pl.ds(first - 1, 1)
        return pl.ds(first, 1), pl.ds(first + size, 1)

    def side_copies(ref, lead, send, recv):
        copies = []
        for k, (dx, dy) in enumerate(SIDES):
            from_x, to_x = window(dx, nx, 1)
            from_y, to_y = window(dy, ny, ROWS)
            copies.append(
                pltpu.make_async_remote_copy(
                    src_ref=ref.at[lead + (from_x, from_y)],
                    dst_ref=ref.at[lead + (to_x, to_y)],
                    send_sem=send(k),
                    recv_sem=recv(k),
                    device_id=device(dx, dy, 0),
                    device_id_type=MESH,
                )
            )
        return copies

    def z_copies(turn, group, rows):
        copies = []
        for k, dz in enumerate((1, -1)):
            copies.append(
                pltpu.make_async_remote_copy(
                    src_ref=packed.at[turn, group, k, pl.ds(0, rows)],
                    dst_ref=landed.at[turn, group, k, pl.ds(0, rows)],
                    send_sem=z_send.at[turn, group, k],
                    recv_sem=z_recv.at[turn, group, k],
                    device_id=device(0, 0, dz),
                    device_id_type=MESH,
                )
            )
        return copies

    started = []

    def start(copies):
        for copy in copies:
            copy.start()
        started.extend(copies)

    def arrive(copies):
        for copy in copies:
            copy.wait_recv()

    def turn_copies(turn):
        ref = (pull0, push0, pull1, push1)[turn]
        copies = side_copies(
            ref, (slice(None),), lambda k: side_send.at[turn, k], lambda k: side_recv.at[turn, k]
        )
        sides = SIDES
        if turn == 0:
            copies += side_copies(act, (), lambda k: act_send.at[k], lambda k: act_recv.at[k])
            sides = SIDES + SIDES
        across = [copy for copy, side in zip(copies, sides) if side[0] != 0]
        along = [copy for copy, side in zip(copies, sides) if side[0] == 0]
        return across, along

    ends = sorted({0, nx - 1})

    def inner_planes(work):
        if nx > 2:
            def step(x, carry):
                work(x)
                return carry
            lax.fori_loop(1, nx - 1, step, 0)

    def own(x, sign):
        inside = [dx for dx in (-1, 0, 1) if 0 <= x - sign * dx < nx]
        return inside, [dx for dx in (-1, 0, 1) if dx not in inside]

    def rolled(value, amount):
        return pltpu.roll(value, amount % nz, 1)

    def prepare(x):
        for j in range(chunks):
            rows, inner = pl.ds(ROWS * j, ROWS), pl.ds(ROWS * (j + 1), ROWS)
            kappa = code[x, rows].astype(jnp.float32) * (1.0 / 1048576.0)
            active = bits[x, rows] * flag[x, rows]
            act[x + 1, inner] = active
            pull0[0, x + 1, inner] = kappa
            for c in range(nf):
                pull0[c + 1, x + 1, inner] = kappa * fields[c, x, rows]
            others = ones_in(jnp.bitwise_and(active, ((1 << 27) - 1) ^ (1 << 13)))
            inverse[x, rows] = 1.0 / (1 + others).astype(jnp.float32)

    loop_planes(nx, prepare)
    packed[...] = jnp.zeros_like(packed)
    pl.semaphore_wait(barrier, len(SIDES) + 2)
    flights = [turn_copies(turn) for turn in range(2 * PASSES)]
    start(flights[0][1])
    start(flights[0][0])

    def pull(step):
        ref = (pull0, pull1)[step]
        target = (push0, push1)[step]
        arrays = range(nf + 1) if step == 0 else range(1, nf + 1)
        turn = 2 * step
        base = 0 if step == 0 else 1
        across, along = flights[turn]

        def sums(x, j, dxs, dzs, found):
            for dx in dxs:
                for dy in (-1, 0, 1):
                    rows = pl.ds(ROWS * (j + 1) - dy, ROWS)
                    active = act[x + 1 - dx, rows]
                    values = [ref[c - base, x + 1 - dx, rows] for c in arrays]
                    for dz in dzs:
                        if (dx, dy, dz) == (0, 0, 0):
                            terms = values
                        else:
                            member = bit_of(active, dx, dy, dz)
                            terms = [jnp.where(member, v, 0.0) for v in values]
                        if dz in found:
                            found[dz] = [a + b for a, b in zip(found[dz], terms)]
                        else:
                            found[dz] = terms
            return found

        def pack(x, j, found):
            rows = pl.ds(ROWS * j, ROWS)
            for k, dz in enumerate((1, -1)):
                tile = packed[turn, 0, k, rows]
                for c, value in zip(arrays, found[dz]):
                    acc[k, c, x, rows] = value
                    at = x * SLOT + c
                    tile = jnp.where(lane == at, rolled(value, at + (dz == 1)), tile)
                packed[turn, 0, k, rows] = tile

        def early(x, dxs, complete):
            for j in range(chunks):
                rows = pl.ds(ROWS * j, ROWS)
                found = sums(x, j, dxs, (1, 0, -1), {})
                for c, value in zip(arrays, found[0]):
                    total[c, x, rows] = value
                if complete:
                    pack(x, j, found)
                else:
                    for k, dz in enumerate((1, -1)):
                        for c, value in zip(arrays, found[dz]):
                            acc[k, c, x, rows] = value

        arrive(along)
        inner_planes(lambda x: early(x, (-1, 0, 1), True))
        for x in ends:
            early(x, own(x, 1)[0], False)
        arrive(across)
        for x in ends:
            for j in range(chunks):
                rows = pl.ds(ROWS * j, ROWS)
                found = {dz: [acc[k, c, x, rows] for c in arrays] for k, dz in enumerate((1, -1))}
                pack(x, j, sums(x, j, own(x, 1)[1], (1, -1), found))
        copies = z_copies(turn, 0, ny)
        start(copies)
        for x in ends:
            for j in range(chunks):
                rows = pl.ds(ROWS * j, ROWS)
                found = {0: [total[c, x, rows] for c in arrays]}
                for c, value in zip(arrays, sums(x, j, own(x, 1)[1], (0,), found)[0]):
                    total[c, x, rows] = value
        arrive(copies)

        def finish(x):
            for j in range(chunks):
                rows, inner = pl.ds(ROWS * j, ROWS), pl.ds(ROWS * (j + 1), ROWS)
                low, high = landed[turn, 0, 0, rows], landed[turn, 0, 1, rows]
                found = {}
                for c in arrays:
                    at = x * SLOT + c
                    from_low = jnp.where(lane == 0, rolled(low, nz - at), rolled(acc[0, c, x, rows], 1))
                    from_high = jnp.where(
                        lane == nz - 1, rolled(high, nz - 1 - at), rolled(acc[1, c, x, rows], nz - 1)
                    )
                    found[c] = total[c, x, rows] + from_low + from_high
                if step == 0:
                    scale = 1.0 / found[0]
                    volume[x, rows] = scale
                else:
                    scale = volume[x, rows]
                for c in range(nf):
                    target[c, x + 1, inner] = found[c + 1] * scale

        for x in ends:
            finish(x)
        start(flights[turn + 1][0])
        inner_planes(finish)
        start(flights[turn + 1][1])

    def push(step):
        ref = (push0, push1)[step]
        turn = 2 * step + 1
        across, along = flights[turn]

        def columns(group, x):
            for j in range(chunks + 2):
                rows = pl.ds(ROWS * j, ROWS)
                for k, dz in enumerate((1, -1)):
                    tile = packed[turn, group, k, rows]
                    for c in range(nf):
                        at = x * SLOT + c
                        tile = jnp.where(lane == at, rolled(ref[c, x, rows], at + (dz == 1)), tile)
                    packed[turn, group, k, rows] = tile

        def shift(group, x):
            for j in range(chunks + 2):
                rows = pl.ds(ROWS * j, ROWS)
                low, high = landed[turn, group, 0, rows], landed[turn, group, 1, rows]
                for c in range(nf):
                    at = x * SLOT + c
                    value = ref[c, x, rows]
                    shifted[0, c, x, rows] = jnp.where(lane == 0, rolled(low, nz - at), rolled(value, 1))
                    shifted[1, c, x, rows] = jnp.where(
                        lane == nz - 1, rolled(high, nz - 1 - at), rolled(value, nz - 1)
                    )

        def planes(first, count, work):
            def step(x, carry):
                work(x)
                return carry
            lax.fori_loop(first, first + count, step, 0)

        def gathered(x, j, dxs, dzs, values):
            active = act[x + 1, pl.ds(ROWS * (j + 1), ROWS)]
            for dz in dzs:
                for dx in dxs:
                    for dy in (-1, 0, 1):
                        rows = pl.ds(ROWS * (j + 1) + dy, ROWS)
                        if dz == 0:
                            terms = [ref[c, x + 1 + dx, rows] for c in range(nf)]
                        else:
                            terms = [shifted[(dz + 1) // 2, c, x + 1 + dx, rows] for c in range(nf)]
                        if (dx, dy, dz) != (0, 0, 0):
                            member = bit_of(active, dx, dy, dz)
                            terms = [jnp.where(member, v, 0.0) for v in terms]
                        values = terms if values is None else [a + b for a, b in zip(values, terms)]
            return values

        def held(x, j):
            return [total[c, x, pl.ds(ROWS * j, ROWS)] for c in range(nf)]

        def keep(x, j, values):
            for c in range(nf):
                total[c, x, pl.ds(ROWS * j, ROWS)] = values[c]

        def give(x, j, values):
            rows, inner = pl.ds(ROWS * j, ROWS), pl.ds(ROWS * (j + 1), ROWS)
            scale = inverse[x, rows]
            if step == PASSES - 1:
                for c in range(nf):
                    out[c, x, rows] = values[c] * scale
            else:
                scale = scale * pull0[0, x + 1, inner]
                for c in range(nf):
                    pull1[c, x + 1, inner] = values[c] * scale

        def add(x, dxs, dzs, first, last):
            for j in range(chunks):
                values = gathered(x, j, dxs, dzs, None if first else held(x, j))
                (give if last else keep)(x, j, values)

        arrive(along)
        planes(1, nx, lambda x: columns(0, x))
        copies = z_copies(turn, 0, ny + 2 * ROWS)
        start(copies)
        inner_planes(lambda x: add(x, (-1, 0, 1), (0,), True, False))
        for x in ends:
            add(x, own(x, -1)[0], (0,), True, False)
        arrive(copies)
        planes(1, nx, lambda x: shift(0, x))
        for x in ends:
            add(x, own(x, -1)[0], (-1, 1), False, False)
        inner_planes(lambda x: add(x, (-1, 0, 1), (-1, 1), False, True))
        arrive(across)
        for x in (0, nx + 1):
            columns(1, x)
        copies = z_copies(turn, 1, ny + 2 * ROWS)
        start(copies)
        for x in ends:
            add(x, own(x, -1)[1], (0,), False, False)
        arrive(copies)
        for x in (0, nx + 1):
            shift(1, x)
        for x in ends:
            add(x, own(x, -1)[1], (-1, 1), False, True)
        if step < PASSES - 1:
            start(flights[turn + 1][1])
            start(flights[turn + 1][0])

    for step in range(PASSES):
        pull(step)
        push(step)
    for copy in started:
        copy.wait_send()


def body(counts, fields, code, flag, bits):
    nf, nx, ny, nz = fields.shape
    frame = (nx + 2, ny + 2 * ROWS, nz)
    turns = 2 * PASSES
    vmem = pl.BlockSpec(memory_space=pltpu.VMEM)
    f32 = jnp.float32
    return pl.pallas_call(
        functools.partial(kernel, counts),
        out_shape=jax.ShapeDtypeStruct(fields.shape, f32),
        in_specs=[vmem] * 4,
        out_specs=vmem,
        scratch_shapes=[
            pltpu.VMEM((nf + 1,) + frame, f32),
            pltpu.VMEM((nf,) + frame, f32),
            pltpu.VMEM((nf,) + frame, f32),
            pltpu.VMEM((nf,) + frame, f32),
            pltpu.VMEM(frame, jnp.int32),
            pltpu.VMEM((nx, ny, nz), f32),
            pltpu.VMEM((nx, ny, nz), f32),
            pltpu.VMEM((2, nf + 1, nx, ny, nz), f32),
            pltpu.VMEM((nf + 1, nx, ny, nz), f32),
            pltpu.VMEM((2, nf) + frame, f32),
            pltpu.VMEM((turns, 2, 2, ny + 2 * ROWS, nz), f32),
            pltpu.VMEM((turns, 2, 2, ny + 2 * ROWS, nz), f32),
            pltpu.SemaphoreType.DMA((turns, len(SIDES))),
            pltpu.SemaphoreType.DMA((turns, len(SIDES))),
            pltpu.SemaphoreType.DMA((len(SIDES),)),
            pltpu.SemaphoreType.DMA((len(SIDES),)),
            pltpu.SemaphoreType.DMA((turns, 2, 2)),
            pltpu.SemaphoreType.DMA((turns, 2, 2)),
        ],
        compiler_params=pltpu.CompilerParams(collective_id=0, has_side_effects=True),
    )(fields, code, flag, bits)


def folded_kernel(
    counts, fields, code, flag, bits, out,
    field_box, code_box, raw, rawcode, bit_box, flag_box, act_box, act, pull0, push0, pull1, push1,
    edge_act, edge0, edge1, edge2, ends, act_ends,
    volume, inverse, weight, edge_volume, edge_weight,
    packed, act_packed, landed, act_landed, done,
    load_sem, x_send, x_recv, y_send, y_recv, z_send, z_recv, back_send, back_recv, token,
):
    nf, nx, ny, nz = fields.shape
    planes = 2 * nx
    half = ny // 2
    tiles = (half + 2 * REACH) // ROWS
    place = [lax.axis_index(name) for name in AXES]
    side = place[0]
    last = ny - REACH
    top, bottom = ROWS, ROWS + REACH + half

    def device(dx, dy, dz):
        step = (dx, dy, dz)
        return tuple(
            lax.rem(place[d] + step[d] + counts[d], counts[d]) if step[d] else place[d]
            for d in range(3)
        )

    def by_side(work):
        for s in (0, 1):
            @pl.when(side == s)
            def _(s=s):
                work(s)

    barrier = pltpu.get_barrier_semaphore()

    row, end_row = place[1], counts[1] - 1
    near = [(1, 0, 0), (0, 0, 1), (0, 0, -1)]
    not_first, not_last = row > 0, row < end_row

    def tell(sem, step):
        pl.semaphore_signal(sem, inc=1, device_id=device(*step), device_id_type=MESH)

    for step in near:
        tell(barrier, step)
    for there, dy in ((not_first, -1), (not_last, 1)):
        pl.when(there)(functools.partial(tell, barrier, (0, dy, 0)))

    rising, falling, across = token.at[0], token.at[1], token.at[2]

    def pass_tokens(hop):
        for sem, first, dy in ((rising, 0, 1), (falling, end_row, -1)):
            @pl.when(row == first + dy * hop)
            def _(sem=sem, dy=dy):
                if hop > 0:
                    pl.semaphore_wait(sem, 1)
                if hop < counts[1] - 1:
                    tell(sem, (0, dy, 0))

    own_planes, far_planes = pl.ds(0, nx), pl.ds(nx, nx)

    def own_rows(s):
        if s == 0:
            return pl.ds(0, half + REACH), pl.ds(ROWS + REACH, half + REACH)
        return pl.ds(half - REACH, half + REACH), pl.ds(ROWS, half + REACH)

    def loads(s):
        box, place_in = own_rows(s)
        return [
            pltpu.make_async_copy(fields, field_box, load_sem.at[4]),
            pltpu.make_async_copy(code, code_box, load_sem.at[5]),
            pltpu.make_async_copy(bits, bit_box, load_sem.at[0]),
            pltpu.make_async_copy(flag, flag_box, load_sem.at[1]),
            pltpu.make_async_copy(fields.at[:, :, box], raw.at[:, own_planes, place_in], load_sem.at[2]),
            pltpu.make_async_copy(code.at[:, box], rawcode.at[own_planes, place_in], load_sem.at[3]),
        ]

    def remote(src, dst, send, recv, step):
        return pltpu.make_async_remote_copy(
            src_ref=src, dst_ref=dst, send_sem=send, recv_sem=recv,
            device_id=device(*step), device_id_type=MESH,
        )

    def triple(from_rows, to_planes, to_rows, send, recv, step):
        return [
            remote(field_box.at[:, :, from_rows], raw.at[:, to_planes, to_rows], send.at[0], recv.at[0], step),
            remote(code_box.at[:, from_rows], rawcode.at[to_planes, to_rows], send.at[1], recv.at[1], step),
            remote(act_box.at[:, from_rows], act.at[0, to_planes, to_rows], send.at[2], recv.at[2], step),
        ]

    def x_rows(s, t):
        if s == 0:
            size = ROWS if t < tiles - 1 else ROWS - REACH
            return pl.ds(half - REACH + ROWS * t, size), pl.ds(ROWS * (t + 1), size)
        if t == 0:
            return pl.ds(0, ROWS - REACH), pl.ds(ROWS + REACH, ROWS - REACH)
        return pl.ds(ROWS * t - REACH, ROWS), pl.ds(ROWS * (t + 1), ROWS)

    def order(s):
        return range(tiles) if s == 1 else range(tiles - 1, -1, -1)

    def x_copies(s, t):
        from_rows, to_rows = x_rows(s, t)
        return triple(from_rows, far_planes, to_rows, x_send.at[t], x_recv.at[t], (1, 0, 0))

    def y_copies(s, cross):
        low, high = pl.ds(0, REACH), pl.ds(last, REACH)
        up = (s == 0) != cross
        rows, to_rows = (high, pl.ds(top, REACH)) if up else (low, pl.ds(bottom, REACH))
        to_planes = far_planes if cross else own_planes
        step = (1 if cross else 0, 1 if up else -1, 0)
        return triple(rows, to_planes, to_rows, y_send.at[int(cross)], y_recv.at[int(cross)], step)

    def z_copies(t):
        rows = pl.ds(pl.multiple_of(ROWS * t, ROWS), ROWS)
        copies = []
        for k, dz in enumerate((1, -1)):
            copies.append(remote(
                packed.at[:, rows], landed.at[k, :, rows], z_send.at[t, k, 0], z_recv.at[t, k, 0], (0, 0, dz),
            ))
            copies.append(remote(
                act_packed.at[rows], act_landed.at[k, rows], z_send.at[t, k, 1], z_recv.at[t, k, 1], (0, 0, dz),
            ))
        return copies

    def box_rows(s, k):
        return pl.ds(pl.multiple_of(s * half + ROWS * k, ROWS), ROWS)

    parts = [(first, size) for first, size in ((0, nx // 2), (nx // 2, nx - nx // 2)) if size]

    def back_copy(k, part):
        some = pl.ds(*parts[part])
        return remote(
            done.at[k, :, some], out.at[:, some, box_rows(side, k)], back_send.at[k, part], back_recv.at[k, part], (1, 0, 0),
        )

    lane = lax.broadcasted_iota(jnp.int32, (ROWS, nz), 1)
    within = jnp.bitwise_and(lane, GROUP - 1)
    member_of = jnp.right_shift(lane, GROUP.bit_length() - 1)

    def rolled(value, amount):
        amount %= nz
        return pltpu.roll(value, amount, 1) if amount else value

    def begin(s):
        copies = loads(s)
        for copy in copies:
            copy.start()
        box, place_in = own_rows(s)
        chunks = [x_copies(s, t) for t in order(1 - s)]
        pl.semaphore_wait(barrier, len(near) + not_first.astype(jnp.int32) + not_last.astype(jnp.int32))
        for copy in copies[:2]:
            copy.wait()
        for copy in chunks[0][:2]:
            copy.start()
        for copy in copies[2:4]:
            copy.wait()

        def plane(x, carry):
            for j in range(ny // ROWS):
                rows = pl.ds(ROWS * j, ROWS)
                act_box[x, rows] = bit_box[x, rows] * flag_box[x, rows]
            return carry

        lax.fori_loop(0, nx, plane, 0, unroll=nx)
        for copy in chunks[0][2:] + sum(chunks[1:], []):
            copy.start()

        for hop in range(counts[1] - 1):
            pass_tokens(hop)

        def keep(x, carry):
            start, end, size = box.start, place_in.start, box.size
            for j in range(0, size, ROWS):
                n = min(ROWS, size - j)
                act[0, x, pl.ds(end + j, n)] = act_box[x, pl.ds(start + j, n)]
            return carry

        lax.fori_loop(0, nx, keep, 0, unroll=nx)
        for copy in copies[4:]:
            copy.wait()

    by_side(begin)

    def arrived(s, t):
        short = t == (tiles - 1) * s

        def wait_rows(size):
            rows = pl.ds(0, size)
            for copy in triple(rows, far_planes, rows, x_send.at[t], x_recv.at[t], (1, 0, 0)):
                copy.wait_recv()

        @pl.when(short)
        def _():
            wait_rows(ROWS - REACH)
            for cross in (False, True):
                for copy in y_copies(0, cross):
                    copy.wait_recv()

        @pl.when(jnp.logical_not(short))
        def _():
            wait_rows(ROWS)

    def view(ref, t, *lead):
        return ref.at[(*lead, pl.ds(pl.multiple_of(ROWS * t, ROWS), 3 * ROWS))]

    def get(ref, t, offset, *lead):
        return view(ref, t, *lead)[pl.ds(offset, ROWS)]

    def put(ref, t, offset, *lead):
        def write(value):
            view(ref, t, *lead)[pl.ds(offset, ROWS)] = value
        return write

    def strip(t):
        return pl.ds(pl.multiple_of(ROWS * t, ROWS), ROWS)

    def prepare(t):
        def plane(x, carry):
            kappa = get(rawcode, t, ROWS, x).astype(jnp.float32) * (1.0 / 1048576.0)
            put(pull0, t, ROWS, 0, x, 0)(kappa)
            for c in range(nf):
                put(pull0, t, ROWS, 0, x, c + 1)(kappa * get(raw, t, ROWS, c, x))
            return carry

        lax.fori_loop(0, planes, plane, 0, unroll=planes)
        for c in range(-1, nf + 1):
            tile = None
            for x in range(planes):
                value = get(act, t, ROWS, 0, x) if c < 0 else get(pull0, t, ROWS, 0, x, c)
                value = rolled(value, GROUP * x + 2 * REACH)
                tile = value if tile is None else jnp.where(member_of == x, value, tile)
            if c < 0:
                act_packed[strip(t)] = tile
            else:
                packed[c, strip(t)] = tile
        for copy in z_copies(t):
            copy.start()

        def counts_of(x, carry):
            others = ones_in(jnp.bitwise_and(get(act, t, ROWS, 0, x), ((1 << 27) - 1) ^ (1 << 13)))
            scale = 1.0 / (1 + others).astype(jnp.float32)
            put(inverse, t, ROWS, x)(scale)
            put(weight, t, ROWS, x)(scale * get(pull0, t, ROWS, 0, x, 0))
            return carry

        lax.fori_loop(0, planes, counts_of, 0, unroll=planes)

    turns = [(sx, sz) for sx in (-1, 0, 1) for sz in (-1, 0, 1)]

    def spread(tile, keep, keep_end):
        for v, (sx, sz) in enumerate(turns if keep else []):
            keep(v)(rolled(tile, -(GROUP * sx + sz)))
        meet = 3 * REACH + 1
        pair = jnp.where(within == meet, rolled(tile, meet - (REACH - 1)), tile)
        for x in range(planes):
            keep_end(x, rolled(pair, -(GROUP * x + meet)))

    def beside(value, end):
        return (
            jnp.where(lane == 0, end, rolled(value, 1)),
            jnp.where(lane == nz - 1, end, rolled(value, -1)),
        )

    def unpack(t):
        for copy in z_copies(t):
            copy.wait_recv()
        at = strip(t)

        def joined(own, low, high):
            left = rolled(jnp.where(within < 2 * REACH, low, own), -REACH)
            right = rolled(jnp.where(within < 2 * REACH, own, high), REACH)
            return jnp.where(within < 2 * REACH, left, right)

        tile = joined(act_packed[at], act_landed[0, at], act_landed[1, at])

        def keep_end(x, value):
            act_ends[x] = value

        spread(tile, lambda v: put(edge_act, t, ROWS, v), keep_end)
        others = ones_in(jnp.bitwise_and(tile, ((1 << 27) - 1) ^ (1 << 13)))
        scale = 1.0 / (1 + others).astype(jnp.float32)
        for c in range(nf + 1):
            tile = joined(packed[c, at], landed[0, c, at], landed[1, c, at])
            if c == 0:
                put(edge_weight, t, ROWS)(scale * tile)

            def keep_end(x, value):
                ends[x, c] = value

            spread(tile, lambda v: put(edge0, t, ROWS, v, c), keep_end)

        def plane(x, carry):
            low, high = beside(get(act, t, ROWS, 0, x), act_ends[x])
            put(act, t, ROWS, 1, x)(low)
            put(act, t, ROWS, 2, x)(high)
            for c in range(nf + 1):
                low, high = beside(get(pull0, t, ROWS, 0, x, c), ends[x, c])
                put(pull0, t, ROWS, 1, x, c)(low)
                put(pull0, t, ROWS, 2, x, c)(high)
            return carry

        lax.fori_loop(0, planes, plane, 0, unroll=planes)

    def gathered(mask_at, value_at, arrays, pulls):
        values = list(value_at(0, 0, 0))
        center = None if pulls else mask_at(0, 0, 0)
        for sx in (-1, 0, 1):
            for sy in (-1, 0, 1):
                for sz in (-1, 0, 1):
                    if (sx, sy, sz) == (0, 0, 0):
                        continue
                    if pulls:
                        member = bit_of(mask_at(sx, sy, sz), -sx, -sy, -sz)
                    else:
                        member = bit_of(center, sx, sy, sz)
                    terms = value_at(sx, sy, sz)
                    values = [a + jnp.where(member, b, 0.0) for a, b in zip(values, terms)]
        return values

    shifts = {0: 0, -1: 1, 1: 2}

    def edge_values(source, arrays, pulls, t, first):
        def mask_at(sx, sy, sz):
            return get(edge_act, t, first + sy, turns.index((sx, sz)))

        def value_at(sx, sy, sz):
            return [get(source, t, first + sy, turns.index((sx, sz)), c) for c in range(arrays)]

        return gathered(mask_at, value_at, arrays, pulls)

    def plane_values(source, arrays, pulls, t, first, x):
        at = {0: x, -1: jnp.where(x == 0, planes - 1, x - 1), 1: jnp.where(x == planes - 1, 0, x + 1)}

        def mask_at(sx, sy, sz):
            return get(act, t, first + sy, shifts[sz], at[sx])

        def value_at(sx, sy, sz):
            return [get(source, t, first + sy, shifts[sz], at[sx], c) for c in range(arrays)]

        return gathered(mask_at, value_at, arrays, pulls)

    def finish(values, stage, read_weight, read_volume, write_volume):
        if stage == 0:
            scale = 1.0 / values[0]
            write_volume(scale)
            values = values[1:]
        elif stage == 1:
            scale = read_weight()
        else:
            scale = read_volume()
        return [value * scale for value in values]

    sources = ((pull0, edge0), (push0, edge1), (pull1, edge2), (push1, None))

    def advance(s, stage, t):
        first = ROWS - 1 - stage if s == 1 else ROWS + 1 + stage
        source, edge_source = sources[stage]
        target, edge_target = sources[stage + 1]
        arrays = nf + 1 if stage == 0 else nf
        pulls = stage % 2 == 0
        values = edge_values(edge_source, arrays, pulls, t, first)
        values = finish(
            values, stage, lambda: get(edge_weight, t, first),
            lambda: get(edge_volume, t, first), put(edge_volume, t, first),
        )
        for c, value in enumerate(values):
            def keep_end(x, moved):
                ends[x, c] = moved

            spread(value, None if stage == 2 else lambda v: put(edge_target, t, first, v, c), keep_end)

        def plane(x, carry):
            values = plane_values(source, arrays, pulls, t, first, x)
            values = finish(
                values, stage, lambda: get(weight, t, first, x),
                lambda: get(volume, t, first, x), put(volume, t, first, x),
            )
            for c, value in enumerate(values):
                low, high = beside(value, ends[x, c])
                put(target, t, first, 0, x, c)(value)
                put(target, t, first, 1, x, c)(low)
                put(target, t, first, 2, x, c)(high)
            return carry

        lax.fori_loop(0, planes, plane, 0, unroll=planes)

    def deliver(s, t):
        k = t - s
        first = REACH if s == 1 else ROWS + REACH
        rows = box_rows(s, k)

        def result(x):
            scale = get(inverse, t, first, x)
            return [value * scale for value in plane_values(push1, nf, False, t, first, x)]

        def far(x, carry):
            for c, value in enumerate(result(nx + x)):
                done[k, c, x] = value
            return carry

        def near(x, carry):
            for c, value in enumerate(result(x)):
                out[c, x, rows] = value
            return carry

        for part, (start, size) in enumerate(parts):
            lax.fori_loop(start, start + size, far, 0, unroll=size)
            back_copy(k, part).start()
        lax.fori_loop(0, nx, near, 0, unroll=nx)

    def run(s):
        def tile(u):
            return u if s == 1 else tiles - 1 - u

        def step(u, carry):
            @pl.when(u < tiles)
            def _():
                arrived(s, tile(u))
                prepare(tile(u))

            @pl.when(u == 0)
            def _():
                pass_tokens(counts[1] - 1)
                tell(across, (1, 0, 0))

            @pl.when(u == 1)
            def _():
                pl.semaphore_wait(across, 1)
                for copy in y_copies(s, False) + y_copies(s, True):
                    copy.start()

            @pl.when(u > 0)
            def _():
                unpack(tile(u - 1))
                for stage in range(3):
                    advance(s, stage, tile(u - 1))

            @pl.when(u > 1)
            def _():
                deliver(s, tile(u - 1))

            return carry

        lax.fori_loop(0, tiles + 1, step, 0)

    by_side(run)

    for t in range(tiles):
        for copy in z_copies(t):
            copy.wait_send()

    def drain(s):
        for copy in y_copies(s, False) + y_copies(s, True):
            copy.wait_send()
        for t in range(tiles):
            for copy in x_copies(s, t):
                copy.wait_send()

    by_side(drain)
    for k in range(tiles - 1):
        for part in range(len(parts)):
            back_copy(k, part).wait()


def folded_body(counts, fields, code, flag, bits):
    nf, nx, ny, nz = fields.shape
    planes = 2 * nx
    depth = ny // 2 + 2 * REACH
    tiles = depth // ROWS
    high = depth + 2 * ROWS
    f32, i32 = jnp.float32, jnp.int32
    whole = pl.BlockSpec(memory_space=pl.ANY)
    dma = pltpu.SemaphoreType.DMA

    def main(n):
        return pltpu.VMEM((3, planes, n, high, nz), f32)

    def edge(n):
        return pltpu.VMEM((9, n, high, nz), f32)

    return pl.pallas_call(
        functools.partial(folded_kernel, counts),
        out_shape=pltpu.VMEM(fields.shape, f32),
        in_specs=[whole] * 4,
        out_specs=pl.BlockSpec(memory_space=pltpu.VMEM),
        scratch_shapes=[
            pltpu.VMEM((nf, nx, ny, nz), f32),
            pltpu.VMEM((nx, ny, nz), i32),
            pltpu.VMEM((nf, planes, high, nz), f32),
            pltpu.VMEM((planes, high, nz), i32),
            pltpu.VMEM((nx, ny, nz), i32),
            pltpu.VMEM((nx, ny, nz), i32),
            pltpu.VMEM((nx, ny, nz), i32),
            pltpu.VMEM((3, planes, high, nz), i32),
            main(nf + 1), main(nf), main(nf), main(nf),
            pltpu.VMEM((9, high, nz), i32),
            edge(nf + 1), edge(nf), edge(nf),
            pltpu.VMEM((planes, nf + 1, ROWS, nz), f32),
            pltpu.VMEM((planes, ROWS, nz), i32),
            pltpu.VMEM((planes, high, nz), f32),
            pltpu.VMEM((planes, high, nz), f32),
            pltpu.VMEM((planes, high, nz), f32),
            pltpu.VMEM((high, nz), f32),
            pltpu.VMEM((high, nz), f32),
            pltpu.VMEM((nf + 1, depth, nz), f32),
            pltpu.VMEM((depth, nz), i32),
            pltpu.VMEM((2, nf + 1, depth, nz), f32),
            pltpu.VMEM((2, depth, nz), i32),
            pltpu.VMEM((tiles - 1, nf, nx, ROWS, nz), f32),
            dma((6,)),
            dma((tiles, 3)), dma((tiles, 3)),
            dma((2, 3)), dma((2, 3)),
            dma((tiles, 2, 2)), dma((tiles, 2, 2)),
            dma((tiles - 1, 2)), dma((tiles - 1, 2)),
            pltpu.SemaphoreType.REGULAR((3,)),
        ],
        compiler_params=pltpu.CompilerParams(collective_id=0, has_side_effects=True),
    )(fields, code, flag, bits)


def any_body(counts, fields, code, flag, bits):
    nf, nx, ny, nz = fields.shape
    folds = (
        counts[0] == 2 and min(counts) > 1
        and 2 * nx * GROUP == nz
        and ny % (2 * ROWS) == 0 and ny // 2 >= REACH and 2 * REACH == ROWS
    )
    return (folded_body if folds else body)(counts, fields, code, flag, bits)


def solution(mesh):
    counts = tuple(mesh.shape[name] for name in AXES)
    spec = P("gx", "gy", "gz")
    whole = P(None, "gx", "gy", "gz")
    return jax.shard_map(
        functools.partial(any_body, counts),
        mesh=mesh,
        in_specs=(whole, spec, spec, spec),
        out_specs=whole,
        check_vma=False,
    )
```
